32 devices in a mesh: rep: 2 (over x), stretch: 2 (over core), tp: 8 (over z, y).
Axes of the slice: x: 2, y: 2, z: 4, core: 2. Of those that a mesh axis runs over, the one named last changes fastest.
Arguments:
- query: bfloat16 [4, 512, 3072], P(('rep', 'stretch'), 'tp'), parts along dimension 0, may hold values from -64 to 64
- stretch_kv: bfloat16 [2, 4, 512, 3072], P(None, ('rep', 'stretch'), 'tp'), parts along dimension 1, may hold values from -6 to 6
- history_kv: bfloat16 [2, 4096, 3072], P(None, ('rep', 'tp')), parts along dimension 1, may hold values from -6 to 6
- block_mask: int32 [4, 4, 8], P(('rep', 'stretch')), parts along dimension 0, may hold values from 0 to 1, as said below
- noise_level: int32 [4], P(('rep', 'stretch')), parts along dimension 0, may hold values from 0 to 999
- history_blocks: int32 [2], P('rep'), parts along dimension 0, may hold values from 1 to 16
- out_weight: bfloat16 [3072, 6144], P(None, 'tp'), may hold values from -0.109375 to 0.109375
- gate_table: float32 [1000, 6144], P(None, 'tp'), may hold values from -6 to 6
Outputs:
- mixed: bfloat16 [4, 512, 6144], P(('rep', 'stretch'), None, 'tp'), parts along dimension 0
The draws below stay inside these ranges and needn't reach their ends.
There are 2 independent parts, one for each index of `rep`. The reference program is written for one: setup_inputs(seed, part) draws one part's arguments, and reference() takes and returns one part's arrays. A program takes and returns all parts, laid end to end along the dimension named above; an argument that names none is the same for every part. Nothing has to cross between parts.
Inputs may be any that keep to these rules, and one draw needn't show every extreme that they name: block_mask[c, i, 4 + i] = 1 for every query block i; block_mask[0, i, j] = 0 for j < 4.
All inputs are finite; a program needn't handle non-finite values.
Results may differ from the reference program's by a relative error of at most 0.0049.
Values may be sent and summed in bfloat16 or wider, within the bound.
A program may use at most 128 MiB of HBM per device.

```python
import math
import jax
import jax.numpy as jnp
from jax import lax

D = 6144
H = 24
HD = 128
LEVELS = 1000
BLK = 128
CT = 512
QB = 4
HIST = 2048


def shared_draws(key):
    query_key = jax.random.fold_in(key, 101)
    history_key = jax.random.fold_in(key, 202)
    feature_width = H * HD
    history = jnp.clip(jax.random.normal(history_key, (2, HIST, feature_width), jnp.float32), -6.0, 6.0)
    queries = jnp.clip(2.0 * jax.random.normal(query_key, (2, CT, feature_width), jnp.float32), -12.0, 12.0)
    return (queries, history)


def draw_query(key, part):
    return shared_draws(key)[0].astype(jnp.bfloat16)


def draw_history_kv(key, part):
    return shared_draws(key)[1].astype(jnp.bfloat16)


def draw_block_mask(key, part):
    raw_bits = jax.random.randint(jax.random.fold_in(key, 404), (2, QB, 2 * QB), 0, 5)
    grid_rows = lax.broadcasted_iota(jnp.int32, (2, QB, 2 * QB), 1)
    grid_cols = lax.broadcasted_iota(jnp.int32, (2, QB, 2 * QB), 2)
    grid_stretches = lax.broadcasted_iota(jnp.int32, (2, QB, 2 * QB), 0)
    block_allow = jnp.where(raw_bits < 3, 1, 0)
    block_allow = jnp.where(grid_cols == grid_rows + QB, 1, block_allow)
    block_allow = jnp.where((grid_stretches == 0) & (grid_cols < QB), 0, block_allow)
    return block_allow.astype(jnp.int32)


def levels(rng, extent, shards, least, high):
    level = 1.0
    for position, parts in shards:
        heights = jax.random.uniform(jax.random.fold_in(jax.random.fold_in(rng, 6), position), (parts,), jnp.float32, least / len(shards), high / len(shards))
        level = level * jnp.repeat(jnp.exp(heights), extent[position] // parts).reshape((-1,) + (1,) * (len(extent) - 1 - position))
    return level


def bell_draw(own_key, dims, width, most, shards=(), kind=jnp.bfloat16):
    values = jax.random.normal(own_key, dims, jnp.float32) * width
    if len(shards) > 0:
        values = levels(own_key, dims, shards, -0.22, 0.18) * values
    return jnp.clip(values, min=-most, max=most).astype(kind)


def setup_inputs(seed: int = 0, part: int = 0) -> dict:
    key_list = jax.random.split(jax.random.key(seed), 9)
    own_keys = jax.random.split(jax.random.fold_in(key_list[8], part), 9)
    return {
        "query": draw_query(jax.random.fold_in(jax.random.fold_in(key_list[8], part), 71), part),
        "stretch_kv": bell_draw(own_keys[1], (2, 2, CT, H * HD), 1.0, 6.0, ((1, 2), (2, 8))),
        "history_kv": draw_history_kv(jax.random.fold_in(jax.random.fold_in(key_list[8], part), 71), part),
        "block_mask": draw_block_mask(jax.random.fold_in(jax.random.fold_in(key_list[8], part), 71), part),
        "noise_level": jax.random.randint(own_keys[4], (2,), 0, LEVELS).astype(jnp.int32),
        "history_blocks": jax.random.randint(own_keys[5], (1,), 1, HIST // BLK + 1).astype(jnp.int32),
        "out_weight": bell_draw(key_list[6], (H * HD, D), (H * HD) ** -0.5, 0.109375, ((1, 8),)),
        "gate_table": bell_draw(key_list[7], (LEVELS, D), 1.0, 6.0, ((1, 8),), jnp.float32),
    }


NEGATIVE = -1e+30

def single_head(triple_args, allowed):
    queries, key_rows, value_rows = triple_args
    scores = jnp.dot(queries, key_rows.T, preferred_element_type=jnp.float32) * (1.0 / math.sqrt(HD))
    scores = jnp.where(allowed, scores, NEGATIVE)
    row_peak = lax.optimization_barrier(jnp.max(scores, axis=1, keepdims=True))
    weights = jnp.where(allowed, jnp.exp(scores - row_peak), 0.0)
    weight_sum = lax.optimization_barrier(jnp.sum(weights, axis=1, keepdims=True))
    output = jnp.dot(weights, value_rows.astype(jnp.float32), precision=lax.Precision.HIGHEST) / weight_sum
    return output.astype(jnp.bfloat16)

def reference(query, stretch_kv, history_kv, block_mask, noise_level, history_blocks, out_weight, gate_table):
    history_live = jnp.arange(HIST, dtype=jnp.int32) < history_blocks[0] * BLK
    results = []
    for stretch_index in range(2):
        if stretch_index == 1:
            older_pair = stretch_kv[:, 0]
        else:
            older_pair = jnp.zeros_like(stretch_kv[:, 0])
        key_rows = jnp.concatenate([history_kv[0], older_pair[0], stretch_kv[0, stretch_index]], 0)
        value_rows = jnp.concatenate([history_kv[1], older_pair[1], stretch_kv[1, stretch_index]], 0)
        fresh = jnp.repeat(jnp.repeat(block_mask[stretch_index] > 0, BLK, axis=0), BLK, axis=1)
        allowed = jnp.concatenate([jnp.broadcast_to(history_live[None, :], (CT, HIST)), fresh], 1)
        key_count = key_rows.shape[0]
        head_queries = jnp.transpose(query[stretch_index].reshape(CT, H, HD), (1, 0, 2))
        head_keys = jnp.transpose(key_rows.reshape(key_count, H, HD), (1, 0, 2))
        head_values = jnp.transpose(value_rows.reshape(key_count, H, HD), (1, 0, 2))
        attended = lax.map(lambda triple_args: single_head(triple_args, allowed), (head_queries, head_keys, head_values))
        attended = jnp.transpose(attended, (1, 0, 2)).reshape(CT, H * HD)
        projected = jnp.dot(attended, out_weight, preferred_element_type=jnp.float32)
        gate_row = gate_table[noise_level[stretch_index]]
        results.append((projected * gate_row[None, :]).astype(jnp.bfloat16))
    return jnp.stack(results, 0)
```

```python
import functools
import math

import jax
import jax.numpy as jnp
from jax import lax
from jax.experimental import pallas as pl
from jax.experimental.pallas import tpu as pltpu
from jax.sharding import PartitionSpec as P

H = 24
HD = 128
BLK = 128


NEGATIVE = -1e30


def shifted(value, axis, steps):
    count = lax.axis_size(axis)
    first, last = (max(0, -steps), min(count, count - steps))
    return lax.ppermute(value, axis, [(source, source + steps) for source in range(first, last)])


def head_block(queries, key_rows, value_rows, allowed):
    key_count = key_rows.shape[0]
    head_count = queries.shape[1]
    key_heads = key_rows.reshape(key_count, head_count, HD)
    scores = jnp.einsum("qhd,khd->qhk", queries, key_heads, preferred_element_type=jnp.float32) * (
        1.0 / math.sqrt(HD)
    )
    scores = jnp.where(allowed[:, None, :], scores, NEGATIVE)
    row_peak = jnp.max(scores, axis=2)
    weights = jnp.where(allowed[:, None, :], jnp.exp(scores - row_peak[:, :, None]), 0.0)
    weight_sum = jnp.sum(weights, axis=2)
    output = None
    value_heads = value_rows.reshape(key_count, head_count, HD).astype(jnp.float32)
    output = jnp.einsum("qhk,khd->qhd", weights, value_heads, precision=lax.Precision.HIGHEST)
    return (row_peak, weight_sum, output)


def combine(earlier, later):
    row_peak = jnp.maximum(earlier[0], later[0])
    scale_one = jnp.exp(earlier[0] - row_peak)
    scale_two = jnp.exp(later[0] - row_peak)
    weight_sum = earlier[1] * scale_one + later[1] * scale_two
    output = None
    output = earlier[2] * scale_one[:, :, None] + later[2] * scale_two[:, :, None]
    return (row_peak, weight_sum, output)


def column_table(columns, block_count):
    return (columns[:, None] == jnp.arange(2 * block_count, dtype=jnp.int32)[None, :]).astype(
        jnp.float32
    )


def attend_all(
    queries,
    query_positions,
    fresh_keys,
    fresh_values,
    fresh_hot,
    mask_table,
    history_pair,
    history_live,
    span,
):
    row_count = queries.shape[0]
    head_count = queries.shape[1]
    block_count = mask_table.shape[0]
    query_hot = (
        (query_positions // BLK)[:, None] == jnp.arange(block_count, dtype=jnp.int32)[None, :]
    ).astype(jnp.float32)
    fresh_allowed = jnp.dot(jnp.dot(query_hot, mask_table), fresh_hot.T) > 0.5
    base_peak = jnp.full((row_count, head_count), NEGATIVE, jnp.float32)
    skipped = (
        base_peak,
        jnp.zeros((row_count, head_count), jnp.float32),
        jnp.zeros((row_count, head_count, HD), jnp.float32),
    )
    result = head_block(queries, fresh_keys, fresh_values, fresh_allowed)
    for sub_block in range(history_pair.shape[1] // span):
        lower_row = sub_block * span
        key_rows = history_pair[0, lower_row : lower_row + span]
        value_rows = history_pair[1, lower_row : lower_row + span]
        live_rows = history_live[lower_row : lower_row + span]
        allowed = jnp.broadcast_to(live_rows[None, :], (row_count, span))
        block_part = lax.cond(
            jnp.any(live_rows),
            lambda: head_block(queries, key_rows, value_rows, allowed),
            lambda: skipped,
        )
        result = combine(result, block_part)
    return result


def on_device(
    query, stretch_kv, history_kv, block_mask, noise_level, history_blocks, out_weight, gate_table
):
    tp_count = lax.axis_size("tp")
    tp_index = lax.axis_index("tp")
    local_rows = query.shape[1]
    feature_width = query.shape[2]
    history_rows = history_kv.shape[1]
    block_count = block_mask.shape[1]
    own_pair = stretch_kv[:, 0]
    older_pair = shifted(own_pair, "stretch", 1)
    mask_table = block_mask[0].astype(jnp.float32)
    live_limit = history_blocks[0] * BLK
    fresh_keys = jnp.concatenate([older_pair[0], own_pair[0]], 0)
    fresh_values = jnp.concatenate([older_pair[1], own_pair[1]], 0)
    own_positions = tp_index * local_rows + jnp.arange(local_rows, dtype=jnp.int32)
    fresh_hot = column_table(
        jnp.concatenate([own_positions // BLK, block_count + own_positions // BLK], 0), block_count
    )
    history_positions = tp_index * history_rows + jnp.arange(history_rows, dtype=jnp.int32)
    history_live = history_positions < live_limit
    piece = lax.all_gather(query[0], "tp", axis=0, tiled=True)
    row_count = piece.shape[0]
    positions = jnp.arange(row_count, dtype=jnp.int32)
    row_peak, weight_sum, output = attend_all(
        piece.reshape(row_count, H, HD),
        positions,
        fresh_keys,
        fresh_values,
        fresh_hot,
        mask_table,
        history_kv,
        history_live,
        BLK,
    )
    got_outputs, got_peaks, got_sums = (
        lax.all_to_all(
            output.reshape(tp_count, local_rows, H, HD),
            "tp",
            split_axis=0,
            concat_axis=0,
            tiled=True,
        ),
        lax.all_to_all(
            row_peak.reshape(tp_count, local_rows, H), "tp", split_axis=0, concat_axis=0, tiled=True
        ),
        lax.all_to_all(
            weight_sum.reshape(tp_count, local_rows, H),
            "tp",
            split_axis=0,
            concat_axis=0,
            tiled=True,
        ),
    )
    overall = jnp.max(got_peaks, axis=0)
    factor = jnp.exp(got_peaks - overall[None])
    merged_sum = jnp.sum(got_sums * factor, axis=0)
    merged = jnp.sum(got_outputs * factor[:, :, :, None], axis=0) / merged_sum[:, :, None]
    attended = merged.reshape(local_rows, feature_width).astype(jnp.bfloat16)
    projected = jnp.dot(
        lax.all_gather(attended, "tp", axis=0, tiled=True),
        out_weight,
        preferred_element_type=jnp.float32,
    )
    level_hot = (jnp.arange(gate_table.shape[0], dtype=jnp.int32) == noise_level[0]).astype(
        jnp.float32
    )[None, :]
    gate_row = jnp.dot(level_hot, gate_table, precision=lax.Precision.HIGHEST)
    return (projected * gate_row).astype(jnp.bfloat16)[None]


MESH = pl.DeviceIdType.MESH
ROWS = (0, 1)
ASKED = (2,)
PIECES = 2
AHEAD = 3
SIDE_AHEAD = 6
THROTTLE = 3
EARLY = 3
COMBINE_LAG = 2
INNER_LAG = 5
RELAY_LAG = 5
OUTER_LAG = 8


def fused_kernel(
    n,
    chunks,
    mask_ref,
    blocks_ref,
    level_ref,
    query_in,
    fresh_in,
    history_in,
    weight_in,
    gate_in,
    out_ref,
    kv,
    queries,
    own_part,
    own_lse,
    part_send,
    part_recv,
    stat_send,
    stat_recv,
    gathered,
    weight,
    gate,
    bias,
    total,
    in_send,
    in_recv,
    fwd_send,
    pass_send,
    pass_recv,
    query_send,
    query_recv,
    swap_send,
    swap_recv,
    gather_send,
    gather_recv,
    local_sem,
    gate_sem,
):
    me = lax.axis_index("tp")
    core = lax.axis_index("stretch")
    twin = {"stretch": 1 - core}
    line = n // 2
    spot, col = me // 2, me % 2
    members = n // 2
    camp = me // members
    seat = me % members
    inner = (spot > 0) & (spot < line - 1)
    mate_spot = spot + 1 - 2 * (spot % 2)
    side_dev = {"tp": me + 1 - 2 * col}
    mate_dev = {"tp": 2 * mate_spot + col}
    mirror_dev = {"tp": 2 * (line - 1 - spot) + col}
    side_seat = seat + 1 - 2 * col
    mate_seat = 2 * (mate_spot % 2) + col
    diagonal_seat = 2 * (mate_spot % 2) + 1 - col

    local_rows = query_in.shape[1]
    history_rows = history_in.shape[1]
    row_count = n * local_rows
    camp_rows = members * local_rows
    camp_history = members * history_rows
    other_base = camp_history
    own_base = camp_history + camp_rows
    block_count = mask_ref.shape[1]
    camp_blocks = block_count // 2
    piece_blocks = block_count // PIECES
    piece_rows = piece_blocks * BLK
    wide = out_ref.shape[2]

    barrier = pltpu.get_barrier_semaphore()
    for offset in range(1, n):
        pl.semaphore_signal(
            barrier, inc=1, device_id={"tp": lax.rem(me + offset, n)}, device_id_type=MESH
        )
    pl.semaphore_signal(barrier, inc=1, device_id=twin, device_id_type=MESH)
    pl.semaphore_wait(barrier, n)

    def remote(source, target, send, recv, device):
        return pltpu.make_async_remote_copy(
            src_ref=source,
            dst_ref=target,
            send_sem=send,
            recv_sem=recv,
            device_id=device,
            device_id_type=MESH,
        )

    def columns(half, j):
        return pl.ds(pl.multiple_of((half * chunks + j) * HD, HD), HD)

    def history_span(source):
        return pl.ds(pl.multiple_of(source * history_rows, history_rows), history_rows)

    def fresh_span(base, source):
        return pl.ds(pl.multiple_of(base + source * local_rows, local_rows), local_rows)

    def query_span(source):
        return pl.ds(
            pl.multiple_of((camp * members + source) * local_rows, local_rows), local_rows
        )

    def places(j, source):
        return (
            kv.at[j, core, history_span(source), :],
            kv.at[j, :, fresh_span(own_base, source), :],
            queries.at[j, query_span(source), :],
        )

    def own_copies(half, j, device, slot, source, kinds):
        cols = columns(half, j)
        origins = (
            history_in.at[core, :, cols],
            fresh_in.at[:, 0, :, cols],
            query_in.at[0, :, cols],
        )
        targets = places(j, source)
        return [
            remote(
                origins[k],
                targets[k],
                in_send.at[k, j, slot],
                in_recv.at[k, j, source],
                device,
            )
            for k in kinds
        ]

    def forward(j, kinds):
        spots = places(j, side_seat)
        return [
            remote(
                spots[k], spots[k], fwd_send.at[k, j], in_recv.at[k, j, side_seat], mate_dev
            )
            for k in kinds
        ]

    def passed_history(j, source, which):
        place = kv.at[j, which, history_span(source), :]
        return remote(
            place, place, pass_send.at[0, j, source], pass_recv.at[0, j, source], twin
        )

    def passed_fresh(j, source):
        return remote(
            kv.at[j, :, fresh_span(own_base, source), :],
            kv.at[j, :, fresh_span(other_base, source), :],
            pass_send.at[1, j, source],
            pass_recv.at[1, j, source],
            twin,
        )

    def own_fresh(j):
        return remote(
            fresh_in.at[:, 0, :, columns(col, j)],
            kv.at[j, :, fresh_span(other_base, seat), :],
            pass_send.at[1, j, seat],
            pass_recv.at[1, j, seat],
            twin,
        )

    def local_copy(j, place):
        cols = columns(col, j)
        source, target = (
            (history_in.at[:, :, cols], kv.at[j, :, history_span(seat), :]),
            (fresh_in.at[:, 0, :, cols], kv.at[j, :, fresh_span(own_base, seat), :]),
            (query_in.at[0, :, cols], queries.at[j, query_span(seat), :]),
            (weight_in.at[:, j], weight.at[j]),
        )[place]
        return pltpu.make_async_copy(source, target, local_sem.at[place, j])

    def mirrored_query(j, which):
        rows = pl.ds(pl.multiple_of(which * camp_rows, camp_rows), camp_rows)
        place = queries.at[j, rows, :]
        return remote(place, place, query_send.at[j], query_recv.at[j], mirror_dev)

    def swapped(j, piece):
        rows = pl.ds(piece * piece_rows, piece_rows)
        return (
            remote(
                part_send.at[j, rows, :],
                part_recv.at[j, rows, :],
                swap_send.at[0, j, piece],
                swap_recv.at[0, j, piece],
                mirror_dev,
            ),
            remote(
                stat_send.at[j, :, rows],
                stat_recv.at[j, :, rows],
                swap_send.at[1, j, piece],
                swap_recv.at[1, j, piece],
                mirror_dev,
            ),
        )

    def spread(half, j, piece):
        place = gathered.at[half * chunks + j, pl.ds(piece * piece_rows, piece_rows), :]
        return [
            remote(
                place,
                place,
                gather_send.at[way, j, piece],
                gather_recv.at[half * chunks + j, piece],
                device,
            )
            for way, device in enumerate((side_dev, mate_dev))
        ]

    def block_rows(block):
        return pl.ds(pl.multiple_of(block * BLK, BLK), BLK)

    gate_copy = pltpu.make_async_copy(gate_in, gate, gate_sem)
    unit = math.log2(math.e) / math.sqrt(HD)

    def prepare_bias():
        live = blocks_ref[0] * BLK
        positions = camp * camp_history + lax.broadcasted_iota(
            jnp.int32, (1, camp_history), 1
        )
        history_bias = jnp.where(positions < live, 0.0, NEGATIVE)
        for block in range(block_count):
            bias[block : block + 1, 0:camp_history] = history_bias
            for part in range(2):
                for near in range(camp_blocks):
                    column = part * block_count + camp * camp_blocks + near
                    shown = jnp.full((1, BLK), mask_ref[0, block, column], jnp.int32)
                    begin = camp_history + part * camp_rows + near * BLK
                    bias[block : block + 1, begin : begin + BLK] = jnp.where(
                        shown > 0, 0.0, NEGATIVE
                    )

    def attend(j, piece):
        rows = pl.ds(piece * piece_rows, piece_rows)
        scores = lax.dot_general(
            queries[j, rows, :],
            kv[j, 0],
            (((1,), (1,)), ((), ())),
            preferred_element_type=jnp.float32,
        )
        peaks, sums, parts = [], [], []
        for place in range(piece_blocks):
            block = piece * piece_blocks + place
            part = scores[place * BLK : (place + 1) * BLK] * unit + bias[block : block + 1, :]
            peak = jnp.max(part, axis=1, keepdims=True)
            part = jnp.exp2(part - peak)
            peaks.append(peak)
            sums.append(jnp.sum(part, axis=1, keepdims=True))
            parts.append(part.astype(jnp.bfloat16))
        output = jnp.dot(
            jnp.concatenate(parts, axis=0), kv[j, 1], preferred_element_type=jnp.float32
        )
        output = output / jnp.concatenate(sums, axis=0)
        own_part[j, rows, :] = output
        part_send[j, rows, :] = output.astype(jnp.bfloat16)
        for place in range(piece_blocks):
            begin = piece * piece_rows + place * BLK
            level = jnp.broadcast_to(peaks[place] + jnp.log2(sums[place]), (BLK, BLK))
            own_lse[j, begin : begin + BLK, :] = level
            stat_send[j, :, begin : begin + BLK] = level.T[0:8, :]

    def combine(j, piece):
        def step(block, carry):
            rows = block_rows(block)
            mine = own_lse[j, rows, :]
            theirs = jnp.broadcast_to(stat_recv[j, 0:1, rows], (BLK, BLK)).T
            top = jnp.maximum(mine, theirs)
            first = jnp.exp2(mine - top)
            second = jnp.exp2(theirs - top)
            mixed = own_part[j, rows, :] * first + part_recv[j, rows, :].astype(
                jnp.float32
            ) * second
            gathered[col * chunks + j, rows, :] = (mixed / (first + second)).astype(
                jnp.bfloat16
            )
            return carry

        lax.fori_loop(piece * piece_blocks, (piece + 1) * piece_blocks, step, 0)

    def project(j, halves, last):
        local_copy(j, 3).wait()
        for piece in range(PIECES):
            for half in halves:
                spread(half, j, piece)[0].wait_recv()

            def step(block, carry):
                rows = block_rows(block)
                left = jnp.concatenate(
                    [gathered[j, rows, :], gathered[chunks + j, rows, :]], axis=1
                )
                right = weight[j].reshape(2 * HD, wide)
                part = jnp.dot(left, right, preferred_element_type=jnp.float32)
                part = part + total[rows, :]
                if last:
                    factor = gate[pl.ds(level_ref[0], 1), :]
                    out_ref[0, rows, :] = (part * factor).astype(out_ref.dtype)
                else:
                    total[rows, :] = part
                return carry

            lax.fori_loop(piece * piece_blocks, (piece + 1) * piece_blocks, step, 0)

    def every(body, count=chunks, first=0):
        def step(j, carry):
            body(j)
            return carry

        lax.fori_loop(first, count, step, 0)

    def start(copies):
        for copy in copies:
            copy.start()

    @pl.when(inner)
    def _():
        def ask(j):
            start(own_copies(1 - col, j, side_dev, 0, seat, ASKED))

        def begin(j):
            start(own_copies(1 - col, j, side_dev, 0, seat, ROWS))
            pl.when(j + EARLY < chunks)(lambda: ask(j + EARLY))

        every(ask, EARLY)
        every(begin, SIDE_AHEAD)

        def fetch(j):
            for place in range(4):
                local_copy(j, place).start()
            own_fresh(j).start()

        every(fetch)
        gate_copy.start()
        total[...] = jnp.zeros_like(total)
        prepare_bias()
        sources = (side_seat, mate_seat, diagonal_seat)

        def answer(j):
            local_copy(j, 2).wait()
            for source in sources:
                own_copies(col, j, side_dev, 0, source, ASKED)[0].wait_recv()
            mirrored_query(j, camp).start()

        every(answer, EARLY)

        def take(j):
            for place in range(2):
                local_copy(j, place).wait()
            for source in sources:
                arrivals = own_copies(col, j, side_dev, 0, source, ROWS)
                arrivals[0].wait_recv()
                passed_history(j, source, core).start()
                arrivals[1].wait_recv()
                passed_fresh(j, source).start()
            pl.when(j + SIDE_AHEAD < chunks)(lambda: begin(j + SIDE_AHEAD))
            pl.when(j + EARLY < chunks)(lambda: answer(j + EARLY))

        def work(j):
            for source in sources:
                passed_history(j, source, 1 - core).wait_recv()
                passed_fresh(j, source).wait_recv()
            own_fresh(j).wait_recv()
            mirrored_query(j, 1 - camp).wait_recv()
            for piece in range(PIECES):
                attend(j, piece)
                start(swapped(j, piece))

        def merge(j):
            for piece in range(PIECES):
                for copy in swapped(j, piece):
                    copy.wait_recv()
                combine(j, piece)
                start(spread(col, j, piece))

        def round_of(step):
            pl.when(step < chunks)(lambda: take(step))
            pl.when((step >= COMBINE_LAG) & (step < chunks + COMBINE_LAG))(
                lambda: merge(step - COMBINE_LAG)
            )
            pl.when(step >= INNER_LAG)(
                lambda: project(step - INNER_LAG, (1 - col,), False)
            )
            pl.when(step < chunks)(lambda: work(step))

        every(round_of, chunks - 1 + INNER_LAG)
        gate_copy.wait()
        project(chunks - 1, (1 - col,), True)

        def drain(j):
            for copy in own_copies(1 - col, j, side_dev, 0, seat, ROWS + ASKED):
                copy.wait_send()
            for source in sources:
                passed_history(j, source, core).wait_send()
                passed_fresh(j, source).wait_send()
            own_fresh(j).wait_send()
            mirrored_query(j, camp).wait_send()
            for piece in range(PIECES):
                for copy in swapped(j, piece):
                    copy.wait_send()
                for copy in spread(col, j, piece):
                    copy.wait_send()

        every(drain)

    @pl.when(jnp.logical_not(inner))
    def _():
        def ask(j):
            start(own_copies(1 - col, j, side_dev, 1, seat, ASKED))
            start(own_copies(col, j, mate_dev, 0, seat, ASKED))

        def begin(j):
            start(own_copies(col, j, mate_dev, 0, seat, ROWS))

        def begin_side(j):
            start(own_copies(1 - col, j, side_dev, 1, seat, ROWS))
            pl.when(j + EARLY < chunks)(lambda: ask(j + EARLY))

        every(ask, EARLY)
        every(begin, AHEAD)
        every(begin_side, SIDE_AHEAD)
        every(lambda j: local_copy(j, 3).start())
        gate_copy.start()
        total[...] = jnp.zeros_like(total)

        def pass_on(j, kinds):
            arrivals = own_copies(col, j, side_dev, 1, side_seat, kinds)
            copies = forward(j, kinds)
            for arrival, copy in zip(arrivals, copies):
                arrival.wait_recv()
                copy.start()

        every(lambda j: pass_on(j, ASKED), EARLY)

        def hand_on(j):
            pass_on(j, ROWS)
            pl.when(j + AHEAD < chunks)(lambda: begin(j + AHEAD))
            pl.when(j + SIDE_AHEAD < chunks)(lambda: begin_side(j + SIDE_AHEAD))
            pl.when(j + EARLY < chunks)(lambda: pass_on(j + EARLY, ASKED))

        def settle(j):
            for copy in forward(j, ROWS + ASKED):
                copy.wait_send()

        def relay(j):
            for piece in range(PIECES):
                copies = spread(col, j, piece)
                copies[0].wait_recv()
                copies[0].start()

        def round_of(step):
            pl.when(step < chunks)(lambda: hand_on(step))
            pl.when((step >= THROTTLE) & (step < chunks + THROTTLE))(
                lambda: settle(step - THROTTLE)
            )
            pl.when((step >= RELAY_LAG) & (step < chunks + RELAY_LAG))(
                lambda: relay(step - RELAY_LAG)
            )
            pl.when(step >= OUTER_LAG)(
                lambda: project(step - OUTER_LAG, (1 - col,), False)
            )

        every(round_of, chunks - 1 + OUTER_LAG)
        gate_copy.wait()
        project(chunks - 1, (1 - col,), True)

        def drain(j):
            for copy in own_copies(col, j, mate_dev, 0, seat, ROWS + ASKED):
                copy.wait_send()
            for copy in own_copies(1 - col, j, side_dev, 1, seat, ROWS + ASKED):
                copy.wait_send()
            for piece in range(PIECES):
                spread(col, j, piece)[0].wait_send()

        every(drain)


def on_device_fused(
    query, stretch_kv, history_kv, block_mask, noise_level, history_blocks, out_weight, gate_table
):
    n = lax.axis_size("tp")
    chunks = H // 2
    local_rows, history_rows = query.shape[1], history_kv.shape[1]
    row_count = n * local_rows
    key_count = (n * history_rows + 2 * row_count) // 2
    wide = out_weight.shape[1]
    block_count = block_mask.shape[1]
    anywhere = pl.BlockSpec(memory_space=pl.ANY)
    scalars = pl.BlockSpec(memory_space=pltpu.SMEM)
    vector = pl.BlockSpec(memory_space=pltpu.VMEM)
    dma = pltpu.SemaphoreType.DMA
    return pl.pallas_call(
        functools.partial(fused_kernel, n, chunks),
        out_shape=jax.ShapeDtypeStruct((1, row_count, wide), jnp.bfloat16),
        in_specs=[scalars, scalars, scalars, anywhere, anywhere, anywhere, anywhere, anywhere],
        out_specs=vector,
        scratch_shapes=[
            pltpu.VMEM((chunks, 2, key_count, HD), jnp.bfloat16),
            pltpu.VMEM((chunks, row_count, HD), jnp.bfloat16),
            pltpu.VMEM((chunks, row_count, HD), jnp.float32),
            pltpu.VMEM((chunks, row_count, HD), jnp.float32),
            pltpu.VMEM((chunks, row_count, HD), jnp.bfloat16),
            pltpu.VMEM((chunks, row_count, HD), jnp.bfloat16),
            pltpu.VMEM((chunks, 8, row_count), jnp.float32),
            pltpu.VMEM((chunks, 8, row_count), jnp.float32),
            pltpu.VMEM((2 * chunks, row_count, HD), jnp.bfloat16),
            pltpu.VMEM((chunks, 2, HD, wide), jnp.bfloat16),
            pltpu.VMEM(gate_table.shape, jnp.float32),
            pltpu.VMEM((block_count, key_count), jnp.float32),
            pltpu.VMEM((row_count, wide), jnp.float32),
            dma((3, chunks, 2)),
            dma((3, chunks, n // 2)),
            dma((3, chunks)),
            dma((2, chunks, n // 2)),
            dma((2, chunks, n // 2)),
            dma((chunks,)),
            dma((chunks,)),
            dma((2, chunks, PIECES)),
            dma((2, chunks, PIECES)),
            dma((2, chunks, PIECES)),
            dma((2 * chunks, PIECES)),
            dma((4, chunks)),
            dma,
        ],
        compiler_params=pltpu.CompilerParams(
            collective_id=0, has_side_effects=True, vmem_limit_bytes=63 * 1024 * 1024
        ),
    )(
        block_mask,
        history_blocks,
        noise_level,
        query,
        stretch_kv,
        history_kv,
        out_weight.reshape(2, chunks, HD, wide),
        gate_table,
    )


def solution(mesh):
    count = mesh.shape["tp"]
    fits = H % 2 == 0 and count // 2 == 4 and count % 2 == 0 and mesh.shape["stretch"] == 2
    return jax.shard_map(
        on_device_fused if fits else on_device,
        mesh=mesh,
        in_specs=(
            P(("rep", "stretch"), "tp", None),
            P(None, ("rep", "stretch"), "tp", None),
            P(None, ("rep", "tp"), None),
            P(("rep", "stretch"), None, None),
            P(("rep", "stretch")),
            P("rep"),
            P(None, "tp"),
            P(None, "tp"),
        ),
        out_specs=P(("rep", "stretch"), None, "tp"),
        check_vma=False,
    )
```

```python
import functools
import math

import jax
import jax.numpy as jnp
from jax import lax
from jax.experimental import pallas as pl
from jax.experimental.pallas import tpu as pltpu
from jax.sharding import PartitionSpec as P

H = 24
HD = 128
BLK = 128


NEGATIVE = -1e30


def shifted(value, axis, steps):
    count = lax.axis_size(axis)
    first, last = (max(0, -steps), min(count, count - steps))
    return lax.ppermute(value, axis, [(source, source + steps) for source in range(first, last)])


def head_block(queries, key_rows, value_rows, allowed):
    key_count = key_rows.shape[0]
    head_count = queries.shape[1]
    key_heads = key_rows.reshape(key_count, head_count, HD)
    scores = jnp.einsum("qhd,khd->qhk", queries, key_heads, preferred_element_type=jnp.float32) * (
        1.0 / math.sqrt(HD)
    )
    scores = jnp.where(allowed[:, None, :], scores, NEGATIVE)
    row_peak = jnp.max(scores, axis=2)
    weights = jnp.where(allowed[:, None, :], jnp.exp(scores - row_peak[:, :, None]), 0.0)
    weight_sum = jnp.sum(weights, axis=2)
    output = None
    value_heads = value_rows.reshape(key_count, head_count, HD).astype(jnp.float32)
    output = jnp.einsum("qhk,khd->qhd", weights, value_heads, precision=lax.Precision.HIGHEST)
    return (row_peak, weight_sum, output)


def combine(earlier, later):
    row_peak = jnp.maximum(earlier[0], later[0])
    scale_one = jnp.exp(earlier[0] - row_peak)
    scale_two = jnp.exp(later[0] - row_peak)
    weight_sum = earlier[1] * scale_one + later[1] * scale_two
    output = None
    output = earlier[2] * scale_one[:, :, None] + later[2] * scale_two[:, :, None]
    return (row_peak, weight_sum, output)


def column_table(columns, block_count):
    return (columns[:, None] == jnp.arange(2 * block_count, dtype=jnp.int32)[None, :]).astype(
        jnp.float32
    )


def attend_all(
    queries,
    query_positions,
    fresh_keys,
    fresh_values,
    fresh_hot,
    mask_table,
    history_pair,
    history_live,
    span,
):
    row_count = queries.shape[0]
    head_count = queries.shape[1]
    block_count = mask_table.shape[0]
    query_hot = (
        (query_positions // BLK)[:, None] == jnp.arange(block_count, dtype=jnp.int32)[None, :]
    ).astype(jnp.float32)
    fresh_allowed = jnp.dot(jnp.dot(query_hot, mask_table), fresh_hot.T) > 0.5
    base_peak = jnp.full((row_count, head_count), NEGATIVE, jnp.float32)
    skipped = (
        base_peak,
        jnp.zeros((row_count, head_count), jnp.float32),
        jnp.zeros((row_count, head_count, HD), jnp.float32),
    )
    result = head_block(queries, fresh_keys, fresh_values, fresh_allowed)
    for sub_block in range(history_pair.shape[1] // span):
        lower_row = sub_block * span
        key_rows = history_pair[0, lower_row : lower_row + span]
        value_rows = history_pair[1, lower_row : lower_row + span]
        live_rows = history_live[lower_row : lower_row + span]
        allowed = jnp.broadcast_to(live_rows[None, :], (row_count, span))
        block_part = lax.cond(
            jnp.any(live_rows),
            lambda: head_block(queries, key_rows, value_rows, allowed),
            lambda: skipped,
        )
        result = combine(result, block_part)
    return result


def on_device(
    query, stretch_kv, history_kv, block_mask, noise_level, history_blocks, out_weight, gate_table
):
    tp_count = lax.axis_size("tp")
    tp_index = lax.axis_index("tp")
    local_rows = query.shape[1]
    feature_width = query.shape[2]
    history_rows = history_kv.shape[1]
    block_count = block_mask.shape[1]
    own_pair = stretch_kv[:, 0]
    older_pair = shifted(own_pair, "stretch", 1)
    mask_table = block_mask[0].astype(jnp.float32)
    live_limit = history_blocks[0] * BLK
    fresh_keys = jnp.concatenate([older_pair[0], own_pair[0]], 0)
    fresh_values = jnp.concatenate([older_pair[1], own_pair[1]], 0)
    own_positions = tp_index * local_rows + jnp.arange(local_rows, dtype=jnp.int32)
    fresh_hot = column_table(
        jnp.concatenate([own_positions // BLK, block_count + own_positions // BLK], 0), block_count
    )
    history_positions = tp_index * history_rows + jnp.arange(history_rows, dtype=jnp.int32)
    history_live = history_positions < live_limit
    piece = lax.all_gather(query[0], "tp", axis=0, tiled=True)
    row_count = piece.shape[0]
    positions = jnp.arange(row_count, dtype=jnp.int32)
    row_peak, weight_sum, output = attend_all(
        piece.reshape(row_count, H, HD),
        positions,
        fresh_keys,
        fresh_values,
        fresh_hot,
        mask_table,
        history_kv,
        history_live,
        BLK,
    )
    got_outputs, got_peaks, got_sums = (
        lax.all_to_all(
            output.reshape(tp_count, local_rows, H, HD),
            "tp",
            split_axis=0,
            concat_axis=0,
            tiled=True,
        ),
        lax.all_to_all(
            row_peak.reshape(tp_count, local_rows, H), "tp", split_axis=0, concat_axis=0, tiled=True
        ),
        lax.all_to_all(
            weight_sum.reshape(tp_count, local_rows, H),
            "tp",
            split_axis=0,
            concat_axis=0,
            tiled=True,
        ),
    )
    overall = jnp.max(got_peaks, axis=0)
    factor = jnp.exp(got_peaks - overall[None])
    merged_sum = jnp.sum(got_sums * factor, axis=0)
    merged = jnp.sum(got_outputs * factor[:, :, :, None], axis=0) / merged_sum[:, :, None]
    attended = merged.reshape(local_rows, feature_width).astype(jnp.bfloat16)
    projected = jnp.dot(
        lax.all_gather(attended, "tp", axis=0, tiled=True),
        out_weight,
        preferred_element_type=jnp.float32,
    )
    level_hot = (jnp.arange(gate_table.shape[0], dtype=jnp.int32) == noise_level[0]).astype(
        jnp.float32
    )[None, :]
    gate_row = jnp.dot(level_hot, gate_table, precision=lax.Precision.HIGHEST)
    return (projected * gate_row).astype(jnp.bfloat16)[None]


MESH = pl.DeviceIdType.MESH
ROWS = (0, 1)
ASKED = (2,)
PIECES = 2
AHEAD = 3
SIDE_AHEAD = 6
THROTTLE = 3
EARLY = 3
COMBINE_LAG = 2
INNER_LAG = 5
RELAY_LAG = 5
OUTER_LAG = 8


def fused_kernel(
    n,
    chunks,
    mask_ref,
    blocks_ref,
    level_ref,
    query_in,
    fresh_in,
    history_in,
    weight_in,
    gate_in,
    out_ref,
    kv,
    queries,
    own_part,
    own_lse,
    part_send,
    part_recv,
    stat_send,
    stat_recv,
    gathered,
    weight,
    gate,
    bias,
    total,
    in_send,
    in_recv,
    forward_send,
    pass_send,
    pass_recv,
    query_send,
    query_recv,
    swap_send,
    swap_recv,
    gather_send,
    gather_recv,
    weight_sem,
    gate_sem,
):
    me = lax.axis_index("tp")
    core = lax.axis_index("stretch")
    twin = {"stretch": 1 - core}
    line = n // 2
    spot, col = me // 2, me % 2
    members = n // 2
    camp = me // members
    seat = me % members
    inner = (spot > 0) & (spot < line - 1)
    mate_spot = spot + 1 - 2 * (spot % 2)
    side_dev = {"tp": me + 1 - 2 * col}
    mate_dev = {"tp": 2 * mate_spot + col}
    mirror_dev = {"tp": 2 * (line - 1 - spot) + col}
    side_seat = seat + 1 - 2 * col

    local_rows = query_in.shape[1]
    history_rows = history_in.shape[1]
    row_count = n * local_rows
    camp_rows = members * local_rows
    camp_history = members * history_rows
    other_base = camp_history
    own_base = camp_history + camp_rows
    block_count = mask_ref.shape[1]
    camp_blocks = block_count // 2
    piece_blocks = block_count // PIECES
    piece_rows = piece_blocks * BLK
    wide = out_ref.shape[2]

    barrier = pltpu.get_barrier_semaphore()
    for offset in range(1, n):
        pl.semaphore_signal(
            barrier, inc=1, device_id={"tp": lax.rem(me + offset, n)}, device_id_type=MESH
        )
    pl.semaphore_signal(barrier, inc=1, device_id=twin, device_id_type=MESH)
    pl.semaphore_wait(barrier, n)

    def remote(source, target, send, recv, device):
        return pltpu.make_async_remote_copy(
            src_ref=source,
            dst_ref=target,
            send_sem=send,
            recv_sem=recv,
            device_id=device,
            device_id_type=MESH,
        )

    def columns(half, j):
        return pl.ds(pl.multiple_of((half * chunks + j) * HD, HD), HD)

    def history_span(source):
        return pl.ds(pl.multiple_of(source * history_rows, history_rows), history_rows)

    def fresh_span(base, source):
        return pl.ds(pl.multiple_of(base + source * local_rows, local_rows), local_rows)

    def query_span(source):
        return pl.ds(
            pl.multiple_of((camp * members + source) * local_rows, local_rows), local_rows
        )

    camp_span = pl.ds(pl.multiple_of(camp * camp_rows, camp_rows), camp_rows)
    far_span = pl.ds(pl.multiple_of((1 - camp) * camp_rows, camp_rows), camp_rows)

    def places(j, source):
        return (
            kv.at[j, core, history_span(source), :],
            kv.at[j, :, fresh_span(own_base, source), :],
            queries.at[j, query_span(source), :],
        )

    def wholes(j):
        return (
            kv.at[j, core, 0:camp_history, :],
            kv.at[j, :, own_base : own_base + camp_rows, :],
            queries.at[j, camp_span, :],
        )

    def origins(half, j):
        cols = columns(half, j)
        return (
            history_in.at[core, :, cols],
            fresh_in.at[:, 0, :, cols],
            query_in.at[0, :, cols],
        )

    def own_copies(half, j, device, slot, source, kinds):
        from_refs, to_refs = origins(half, j), places(j, source)
        return [
            remote(from_refs[k], to_refs[k], in_send.at[k, slot], in_recv.at[k, j], device)
            for k in kinds
        ]

    def forward(j, kinds):
        spots = places(j, side_seat)
        return [
            remote(spots[k], spots[k], forward_send.at[k, j], in_recv.at[k, j], mate_dev)
            for k in kinds
        ]

    def local_copies(j):
        from_refs, to_refs = origins(col, j), places(j, seat)
        return [
            pltpu.make_async_copy(from_refs[k], to_refs[k], in_recv.at[k, j]) for k in range(3)
        ]

    def await_bytes(ref, sem):
        pltpu.make_async_copy(ref, ref, sem).wait()

    def passed_history(j, which):
        place = kv.at[j, which, 0:camp_history, :]
        return remote(place, place, pass_send.at[0], pass_recv.at[0, j], twin)

    def passed_fresh(j):
        return remote(
            kv.at[j, :, own_base : own_base + camp_rows, :],
            kv.at[j, :, other_base : other_base + camp_rows, :],
            pass_send.at[1],
            pass_recv.at[1, j],
            twin,
        )

    def mirrored_query(j, span):
        place = queries.at[j, span, :]
        return remote(place, place, query_send, query_recv.at[j], mirror_dev)

    def swapped(j, piece):
        rows = pl.ds(piece * piece_rows, piece_rows)
        return (
            remote(
                part_send.at[j, rows, :],
                part_recv.at[j, rows, :],
                swap_send.at[0],
                swap_recv.at[0, j, piece],
                mirror_dev,
            ),
            remote(
                stat_send.at[j, :, rows],
                stat_recv.at[j, :, rows],
                swap_send.at[1],
                swap_recv.at[1, j, piece],
                mirror_dev,
            ),
        )

    def spread(half, j, piece):
        place = gathered.at[half * chunks + j, pl.ds(piece * piece_rows, piece_rows), :]
        return [
            remote(
                place,
                place,
                gather_send.at[way],
                gather_recv.at[half * chunks + j, piece],
                device,
            )
            for way, device in enumerate((side_dev, mate_dev))
        ]

    def block_rows(block):
        return pl.ds(pl.multiple_of(block * BLK, BLK), BLK)

    gate_copy = pltpu.make_async_copy(gate_in, gate, gate_sem)
    unit = math.log2(math.e) / math.sqrt(HD)

    def prepare_bias():
        live = blocks_ref[0] * BLK
        positions = camp * camp_history + lax.broadcasted_iota(
            jnp.int32, (1, camp_history), 1
        )
        history_bias = jnp.where(positions < live, 0.0, NEGATIVE)
        for block in range(block_count):
            bias[block : block + 1, 0:camp_history] = history_bias
            for part in range(2):
                for near in range(camp_blocks):
                    column = part * block_count + camp * camp_blocks + near
                    shown = jnp.full((1, BLK), mask_ref[0, block, column], jnp.int32)
                    begin = camp_history + part * camp_rows + near * BLK
                    bias[block : block + 1, begin : begin + BLK] = jnp.where(
                        shown > 0, 0.0, NEGATIVE
                    )

    def attend(j, piece):
        rows = pl.ds(piece * piece_rows, piece_rows)
        scores = lax.dot_general(
            queries[j, rows, :],
            kv[j, 0],
            (((1,), (1,)), ((), ())),
            preferred_element_type=jnp.float32,
        )
        peaks, sums, parts = [], [], []
        for place in range(piece_blocks):
            block = piece * piece_blocks + place
            part = scores[place * BLK : (place + 1) * BLK] * unit + bias[block : block + 1, :]
            peak = jnp.max(part, axis=1, keepdims=True)
            part = jnp.exp2(part - peak)
            peaks.append(peak)
            sums.append(jnp.sum(part, axis=1, keepdims=True))
            parts.append(part.astype(jnp.bfloat16))
        output = jnp.dot(
            jnp.concatenate(parts, axis=0), kv[j, 1], preferred_element_type=jnp.float32
        )
        output = output / jnp.concatenate(sums, axis=0)
        own_part[j, rows, :] = output
        part_send[j, rows, :] = output.astype(jnp.bfloat16)
        for place in range(piece_blocks):
            begin = piece * piece_rows + place * BLK
            level = jnp.broadcast_to(peaks[place] + jnp.log2(sums[place]), (BLK, BLK))
            own_lse[j, begin : begin + BLK, :] = level
            stat_send[j, :, begin : begin + BLK] = level.T[0:8, :]

    def combine(j, piece):
        def step(block, carry):
            rows = block_rows(block)
            mine = own_lse[j, rows, :]
            theirs = jnp.broadcast_to(stat_recv[j, 0:1, rows], (BLK, BLK)).T
            top = jnp.maximum(mine, theirs)
            first = jnp.exp2(mine - top)
            second = jnp.exp2(theirs - top)
            mixed = own_part[j, rows, :] * first + part_recv[j, rows, :].astype(
                jnp.float32
            ) * second
            gathered[col * chunks + j, rows, :] = (mixed / (first + second)).astype(
                jnp.bfloat16
            )
            return carry

        lax.fori_loop(piece * piece_blocks, (piece + 1) * piece_blocks, step, 0)

    def project(j, halves, last):
        for piece in range(PIECES):
            for half in halves:
                spread(half, j, piece)[0].wait_recv()

            def step(block, carry):
                rows = block_rows(block)
                left = jnp.concatenate(
                    [gathered[j, rows, :], gathered[chunks + j, rows, :]], axis=1
                )
                right = jnp.concatenate([weight[0, j], weight[1, j]], axis=0)
                part = jnp.dot(left, right, preferred_element_type=jnp.float32)
                part = part + total[rows, :]
                if last:
                    factor = gate[pl.ds(level_ref[0], 1), :]
                    out_ref[0, rows, :] = (part * factor).astype(out_ref.dtype)
                else:
                    total[rows, :] = part
                return carry

            lax.fori_loop(piece * piece_blocks, (piece + 1) * piece_blocks, step, 0)

    def every(body, count=chunks, first=0):
        def step(j, carry):
            body(j)
            return carry

        lax.fori_loop(first, count, step, 0)

    def start(copies):
        for copy in copies:
            copy.start()

    weight_copy = pltpu.make_async_copy(weight_in, weight, weight_sem)
    own_half = gathered.at[pl.ds(pl.multiple_of(col * chunks, chunks), chunks)]

    def await_own(slot):
        await_bytes(kv.at[:, 0, 0:history_rows, :], in_send.at[0, slot])
        await_bytes(kv.at[:, :, 0:local_rows, :], in_send.at[1, slot])
        await_bytes(queries.at[:, 0:local_rows, :], in_send.at[2, slot])

    @pl.when(inner)
    def _():
        def ask(j):
            start(own_copies(1 - col, j, side_dev, 0, seat, ASKED))

        def begin(j):
            start(own_copies(1 - col, j, side_dev, 0, seat, ROWS))
            pl.when(j + EARLY < chunks)(lambda: ask(j + EARLY))

        every(ask, EARLY)
        every(begin, SIDE_AHEAD)
        every(lambda j: start(local_copies(j)))
        weight_copy.start()
        gate_copy.start()
        total[...] = jnp.zeros_like(total)
        prepare_bias()

        def answer(j):
            await_bytes(wholes(j)[2], in_recv.at[2, j])
            mirrored_query(j, camp_span).start()

        every(answer, EARLY)

        def take(j):
            await_bytes(wholes(j)[0], in_recv.at[0, j])
            passed_history(j, core).start()
            await_bytes(wholes(j)[1], in_recv.at[1, j])
            passed_fresh(j).start()
            pl.when(j + SIDE_AHEAD < chunks)(lambda: begin(j + SIDE_AHEAD))
            pl.when(j + EARLY < chunks)(lambda: answer(j + EARLY))

        def work(j):
            mirrored_query(j, far_span).wait_recv()
            passed_history(j, 1 - core).wait_recv()
            passed_fresh(j).wait_recv()
            for piece in range(PIECES):
                attend(j, piece)
                start(swapped(j, piece))

        def merge(j):
            for piece in range(PIECES):
                for copy in swapped(j, piece):
                    copy.wait_recv()
                combine(j, piece)
                start(spread(col, j, piece))

        def round_of(step):
            pl.when(step == INNER_LAG)(weight_copy.wait)
            pl.when(step < chunks)(lambda: take(step))
            pl.when((step >= COMBINE_LAG) & (step < chunks + COMBINE_LAG))(
                lambda: merge(step - COMBINE_LAG)
            )
            pl.when(step >= INNER_LAG)(
                lambda: project(step - INNER_LAG, (1 - col,), False)
            )
            pl.when(step < chunks)(lambda: work(step))

        every(round_of, chunks - 1 + INNER_LAG)
        gate_copy.wait()
        project(chunks - 1, (1 - col,), True)
        await_own(0)
        await_bytes(kv.at[:, 0, 0:camp_history, :], pass_send.at[0])
        await_bytes(kv.at[:, :, 0:camp_rows, :], pass_send.at[1])
        await_bytes(queries.at[:, 0:camp_rows, :], query_send)
        await_bytes(part_send, swap_send.at[0])
        await_bytes(stat_send, swap_send.at[1])
        await_bytes(own_half, gather_send.at[0])
        await_bytes(own_half, gather_send.at[1])

    @pl.when(jnp.logical_not(inner))
    def _():
        def ask(j):
            start(own_copies(1 - col, j, side_dev, 1, seat, ASKED))
            start(own_copies(col, j, mate_dev, 0, seat, ASKED))

        def begin(j):
            start(own_copies(col, j, mate_dev, 0, seat, ROWS))

        def begin_side(j):
            start(own_copies(1 - col, j, side_dev, 1, seat, ROWS))
            pl.when(j + EARLY < chunks)(lambda: ask(j + EARLY))

        every(ask, EARLY)
        every(begin, AHEAD)
        every(begin_side, SIDE_AHEAD)
        weight_copy.start()
        gate_copy.start()
        total[...] = jnp.zeros_like(total)

        def pass_on(j, kinds):
            arrivals = own_copies(col, j, side_dev, 1, side_seat, kinds)
            copies = forward(j, kinds)
            for arrival, copy in zip(arrivals, copies):
                arrival.wait_recv()
                copy.start()

        every(lambda j: pass_on(j, ASKED), EARLY)

        def hand_on(j):
            pass_on(j, ROWS)
            pl.when(j + AHEAD < chunks)(lambda: begin(j + AHEAD))
            pl.when(j + SIDE_AHEAD < chunks)(lambda: begin_side(j + SIDE_AHEAD))
            pl.when(j + EARLY < chunks)(lambda: pass_on(j + EARLY, ASKED))

        def settle(j):
            for copy in forward(j, ROWS + ASKED):
                copy.wait_send()

        def relay(j):
            for piece in range(PIECES):
                copy = spread(col, j, piece)[0]
                copy.wait_recv()
                copy.start()

        def round_of(step):
            pl.when(step == OUTER_LAG)(weight_copy.wait)
            pl.when(step < chunks)(lambda: hand_on(step))
            pl.when((step >= THROTTLE) & (step < chunks + THROTTLE))(
                lambda: settle(step - THROTTLE)
            )
            pl.when((step >= RELAY_LAG) & (step < chunks + RELAY_LAG))(
                lambda: relay(step - RELAY_LAG)
            )
            pl.when(step >= OUTER_LAG)(
                lambda: project(step - OUTER_LAG, (1 - col,), False)
            )

        every(round_of, chunks - 1 + OUTER_LAG)
        gate_copy.wait()
        project(chunks - 1, (1 - col,), True)
        await_own(0)
        await_own(1)
        await_bytes(own_half, gather_send.at[0])


def on_device_fused(
    query, stretch_kv, history_kv, block_mask, noise_level, history_blocks, out_weight, gate_table
):
    n = lax.axis_size("tp")
    chunks = H // 2
    local_rows, history_rows = query.shape[1], history_kv.shape[1]
    row_count = n * local_rows
    key_count = (n * history_rows + 2 * row_count) // 2
    wide = out_weight.shape[1]
    block_count = block_mask.shape[1]
    anywhere = pl.BlockSpec(memory_space=pl.ANY)
    scalars = pl.BlockSpec(memory_space=pltpu.SMEM)
    vector = pl.BlockSpec(memory_space=pltpu.VMEM)
    dma = pltpu.SemaphoreType.DMA
    return pl.pallas_call(
        functools.partial(fused_kernel, n, chunks),
        out_shape=jax.ShapeDtypeStruct((1, row_count, wide), jnp.bfloat16),
        in_specs=[scalars, scalars, scalars, anywhere, anywhere, anywhere, anywhere, anywhere],
        out_specs=vector,
        scratch_shapes=[
            pltpu.VMEM((chunks, 2, key_count, HD), jnp.bfloat16),
            pltpu.VMEM((chunks, row_count, HD), jnp.bfloat16),
            pltpu.VMEM((chunks, row_count, HD), jnp.float32),
            pltpu.VMEM((chunks, row_count, HD), jnp.float32),
            pltpu.VMEM((chunks, row_count, HD), jnp.bfloat16),
            pltpu.VMEM((chunks, row_count, HD), jnp.bfloat16),
            pltpu.VMEM((chunks, 8, row_count), jnp.float32),
            pltpu.VMEM((chunks, 8, row_count), jnp.float32),
            pltpu.VMEM((2 * chunks, row_count, HD), jnp.bfloat16),
            pltpu.VMEM((2, chunks, HD, wide), jnp.bfloat16),
            pltpu.VMEM(gate_table.shape, jnp.float32),
            pltpu.VMEM((block_count, key_count), jnp.float32),
            pltpu.VMEM((row_count, wide), jnp.float32),
            dma((3, 2)),
            dma((3, chunks)),
            dma((3, chunks)),
            dma((2,)),
            dma((2, chunks)),
            dma,
            dma((chunks,)),
            dma((2,)),
            dma((2, chunks, PIECES)),
            dma((2,)),
            dma((2 * chunks, PIECES)),
            dma,
            dma,
        ],
        compiler_params=pltpu.CompilerParams(
            collective_id=0, has_side_effects=True, vmem_limit_bytes=63 * 1024 * 1024
        ),
    )(
        block_mask,
        history_blocks,
        noise_level,
        query,
        stretch_kv,
        history_kv,
        out_weight.reshape(2, chunks, HD, wide),
        gate_table,
    )


def solution(mesh):
    count = mesh.shape["tp"]
    fits = H % 2 == 0 and count // 2 == 4 and count % 2 == 0 and mesh.shape["stretch"] == 2
    return jax.shard_map(
        on_device_fused if fits else on_device,
        mesh=mesh,
        in_specs=(
            P(("rep", "stretch"), "tp", None),
            P(None, ("rep", "stretch"), "tp", None),
            P(None, ("rep", "tp"), None),
            P(("rep", "stretch"), None, None),
            P(("rep", "stretch")),
            P("rep"),
            P(None, "tp"),
            P(None, "tp"),
        ),
        out_specs=P(("rep", "stretch"), None, "tp"),
        check_vma=False,
    )
```

```python
import functools
import math

import jax
import jax.numpy as jnp
from jax import lax
from jax.experimental import pallas as pl
from jax.experimental.pallas import tpu as pltpu
from jax.sharding import PartitionSpec as P

H = 24
HD = 128
BLK = 128


NEGATIVE = -1e30


def shifted(value, axis, steps):
    count = lax.axis_size(axis)
    first, last = (max(0, -steps), min(count, count - steps))
    return lax.ppermute(value, axis, [(source, source + steps) for source in range(first, last)])


def head_block(queries, key_rows, value_rows, allowed):
    key_count = key_rows.shape[0]
    head_count = queries.shape[1]
    key_heads = key_rows.reshape(key_count, head_count, HD)
    scores = jnp.einsum("qhd,khd->qhk", queries, key_heads, preferred_element_type=jnp.float32) * (
        1.0 / math.sqrt(HD)
    )
    scores = jnp.where(allowed[:, None, :], scores, NEGATIVE)
    row_peak = jnp.max(scores, axis=2)
    weights = jnp.where(allowed[:, None, :], jnp.exp(scores - row_peak[:, :, None]), 0.0)
    weight_sum = jnp.sum(weights, axis=2)
    output = None
    value_heads = value_rows.reshape(key_count, head_count, HD).astype(jnp.float32)
    output = jnp.einsum("qhk,khd->qhd", weights, value_heads, precision=lax.Precision.HIGHEST)
    return (row_peak, weight_sum, output)


def combine(earlier, later):
    row_peak = jnp.maximum(earlier[0], later[0])
    scale_one = jnp.exp(earlier[0] - row_peak)
    scale_two = jnp.exp(later[0] - row_peak)
    weight_sum = earlier[1] * scale_one + later[1] * scale_two
    output = None
    output = earlier[2] * scale_one[:, :, None] + later[2] * scale_two[:, :, None]
    return (row_peak, weight_sum, output)


def column_table(columns, block_count):
    return (columns[:, None] == jnp.arange(2 * block_count, dtype=jnp.int32)[None, :]).astype(
        jnp.float32
    )


def attend_all(
    queries,
    query_positions,
    fresh_keys,
    fresh_values,
    fresh_hot,
    mask_table,
    history_pair,
    history_live,
    span,
):
    row_count = queries.shape[0]
    head_count = queries.shape[1]
    block_count = mask_table.shape[0]
    query_hot = (
        (query_positions // BLK)[:, None] == jnp.arange(block_count, dtype=jnp.int32)[None, :]
    ).astype(jnp.float32)
    fresh_allowed = jnp.dot(jnp.dot(query_hot, mask_table), fresh_hot.T) > 0.5
    base_peak = jnp.full((row_count, head_count), NEGATIVE, jnp.float32)
    skipped = (
        base_peak,
        jnp.zeros((row_count, head_count), jnp.float32),
        jnp.zeros((row_count, head_count, HD), jnp.float32),
    )
    result = head_block(queries, fresh_keys, fresh_values, fresh_allowed)
    for sub_block in range(history_pair.shape[1] // span):
        lower_row = sub_block * span
        key_rows = history_pair[0, lower_row : lower_row + span]
        value_rows = history_pair[1, lower_row : lower_row + span]
        live_rows = history_live[lower_row : lower_row + span]
        allowed = jnp.broadcast_to(live_rows[None, :], (row_count, span))
        block_part = lax.cond(
            jnp.any(live_rows),
            lambda: head_block(queries, key_rows, value_rows, allowed),
            lambda: skipped,
        )
        result = combine(result, block_part)
    return result


def on_device(
    query, stretch_kv, history_kv, block_mask, noise_level, history_blocks, out_weight, gate_table
):
    tp_count = lax.axis_size("tp")
    tp_index = lax.axis_index("tp")
    local_rows = query.shape[1]
    feature_width = query.shape[2]
    history_rows = history_kv.shape[1]
    block_count = block_mask.shape[1]
    own_pair = stretch_kv[:, 0]
    older_pair = shifted(own_pair, "stretch", 1)
    mask_table = block_mask[0].astype(jnp.float32)
    live_limit = history_blocks[0] * BLK
    fresh_keys = jnp.concatenate([older_pair[0], own_pair[0]], 0)
    fresh_values = jnp.concatenate([older_pair[1], own_pair[1]], 0)
    own_positions = tp_index * local_rows + jnp.arange(local_rows, dtype=jnp.int32)
    fresh_hot = column_table(
        jnp.concatenate([own_positions // BLK, block_count + own_positions // BLK], 0), block_count
    )
    history_positions = tp_index * history_rows + jnp.arange(history_rows, dtype=jnp.int32)
    history_live = history_positions < live_limit
    piece = lax.all_gather(query[0], "tp", axis=0, tiled=True)
    row_count = piece.shape[0]
    positions = jnp.arange(row_count, dtype=jnp.int32)
    row_peak, weight_sum, output = attend_all(
        piece.reshape(row_count, H, HD),
        positions,
        fresh_keys,
        fresh_values,
        fresh_hot,
        mask_table,
        history_kv,
        history_live,
        BLK,
    )
    got_outputs, got_peaks, got_sums = (
        lax.all_to_all(
            output.reshape(tp_count, local_rows, H, HD),
            "tp",
            split_axis=0,
            concat_axis=0,
            tiled=True,
        ),
        lax.all_to_all(
            row_peak.reshape(tp_count, local_rows, H), "tp", split_axis=0, concat_axis=0, tiled=True
        ),
        lax.all_to_all(
            weight_sum.reshape(tp_count, local_rows, H),
            "tp",
            split_axis=0,
            concat_axis=0,
            tiled=True,
        ),
    )
    overall = jnp.max(got_peaks, axis=0)
    factor = jnp.exp(got_peaks - overall[None])
    merged_sum = jnp.sum(got_sums * factor, axis=0)
    merged = jnp.sum(got_outputs * factor[:, :, :, None], axis=0) / merged_sum[:, :, None]
    attended = merged.reshape(local_rows, feature_width).astype(jnp.bfloat16)
    projected = jnp.dot(
        lax.all_gather(attended, "tp", axis=0, tiled=True),
        out_weight,
        preferred_element_type=jnp.float32,
    )
    level_hot = (jnp.arange(gate_table.shape[0], dtype=jnp.int32) == noise_level[0]).astype(
        jnp.float32
    )[None, :]
    gate_row = jnp.dot(level_hot, gate_table, precision=lax.Precision.HIGHEST)
    return (projected * gate_row).astype(jnp.bfloat16)[None]


MESH = pl.DeviceIdType.MESH
ROWS = (0, 1)
ASKED = (2,)
PIECES = 2
AHEAD = 1
SIDE_AHEAD = 6
THROTTLE = 2
EARLY = 5
COMBINE_LAG = 2
INNER_LAG = 5
RELAY_LAG = 5
OUTER_LAG = 8


def fused_kernel(
    n,
    chunks,
    mask_in,
    blocks_in,
    level_in,
    query_in,
    fresh_in,
    history_in,
    weight_in,
    gate_in,
    out_ref,
    kv,
    queries,
    own_part,
    own_lse,
    part_send,
    part_recv,
    stat_send,
    stat_recv,
    gathered,
    weight,
    gate,
    bias,
    total,
    mask_ref,
    blocks_ref,
    level_ref,
    in_send,
    in_recv,
    forward_send,
    pass_send,
    pass_recv,
    query_send,
    query_recv,
    swap_send,
    swap_recv,
    gather_send,
    gather_recv,
    weight_sem,
    gate_sem,
    scalar_sem,
):
    me = lax.axis_index("tp")
    core = lax.axis_index("stretch")
    twin = {"stretch": 1 - core}
    line = n // 2
    spot, col = me // 2, me % 2
    members = n // 2
    camp = me // members
    seat = me % members
    inner = (spot > 0) & (spot < line - 1)
    mate_spot = spot + 1 - 2 * (spot % 2)
    side_dev = {"tp": me + 1 - 2 * col}
    mate_dev = {"tp": 2 * mate_spot + col}
    mirror_dev = {"tp": 2 * (line - 1 - spot) + col}
    side_seat = seat + 1 - 2 * col

    local_rows = query_in.shape[1]
    history_rows = history_in.shape[1]
    row_count = n * local_rows
    camp_rows = members * local_rows
    camp_history = members * history_rows
    other_base = camp_history
    own_base = camp_history + camp_rows
    block_count = mask_in.shape[1]
    camp_blocks = block_count // 2
    piece_blocks = block_count // PIECES
    piece_rows = piece_blocks * BLK
    wide = out_ref.shape[2]

    barrier = pltpu.get_barrier_semaphore()
    for offset in range(1, n):
        pl.semaphore_signal(
            barrier, inc=1, device_id={"tp": lax.rem(me + offset, n)}, device_id_type=MESH
        )
    pl.semaphore_signal(barrier, inc=1, device_id=twin, device_id_type=MESH)
    pl.semaphore_wait(barrier, n)

    def remote(source, target, send, recv, device):
        return pltpu.make_async_remote_copy(
            src_ref=source,
            dst_ref=target,
            send_sem=send,
            recv_sem=recv,
            device_id=device,
            device_id_type=MESH,
        )

    def columns(half, j):
        return pl.ds(pl.multiple_of((half * chunks + j) * HD, HD), HD)

    def history_span(source):
        return pl.ds(pl.multiple_of(source * history_rows, history_rows), history_rows)

    def fresh_span(base, source):
        return pl.ds(pl.multiple_of(base + source * local_rows, local_rows), local_rows)

    def query_span(source):
        return pl.ds(
            pl.multiple_of((camp * members + source) * local_rows, local_rows), local_rows
        )

    camp_span = pl.ds(pl.multiple_of(camp * camp_rows, camp_rows), camp_rows)
    far_span = pl.ds(pl.multiple_of((1 - camp) * camp_rows, camp_rows), camp_rows)

    def places(j, source):
        return (
            kv.at[j, core, history_span(source), :],
            kv.at[j, :, fresh_span(own_base, source), :],
            queries.at[j, query_span(source), :],
        )

    def wholes(j):
        return (
            kv.at[j, core, 0:camp_history, :],
            kv.at[j, :, own_base : own_base + camp_rows, :],
            queries.at[j, camp_span, :],
        )

    def origins(half, j):
        cols = columns(half, j)
        return (
            history_in.at[core, :, cols],
            fresh_in.at[:, 0, :, cols],
            query_in.at[0, :, cols],
        )

    def own_copies(half, j, device, slot, source, kinds):
        from_refs, to_refs = origins(half, j), places(j, source)
        return [
            remote(from_refs[k], to_refs[k], in_send.at[k, slot], in_recv.at[k, j], device)
            for k in kinds
        ]

    def forward(j, kinds):
        spots = places(j, side_seat)
        return [
            remote(spots[k], spots[k], forward_send.at[k, j], in_recv.at[k, j], mate_dev)
            for k in kinds
        ]

    def local_copies(j):
        from_refs, to_refs = origins(col, j), places(j, seat)
        return [
            pltpu.make_async_copy(from_refs[k], to_refs[k], in_recv.at[k, j]) for k in range(3)
        ]

    def await_bytes(ref, sem):
        pltpu.make_async_copy(ref, ref, sem).wait()

    def passed_history(j, which):
        place = kv.at[j, which, 0:camp_history, :]
        return remote(place, place, pass_send.at[0], pass_recv.at[0, j], twin)

    def passed_fresh(j):
        return remote(
            kv.at[j, :, own_base : own_base + camp_rows, :],
            kv.at[j, :, other_base : other_base + camp_rows, :],
            pass_send.at[1],
            pass_recv.at[1, j],
            twin,
        )

    def mirrored_query(j, span):
        place = queries.at[j, span, :]
        return remote(place, place, query_send, query_recv.at[j], mirror_dev)

    def swapped(j, piece):
        rows = pl.ds(piece * piece_rows, piece_rows)
        return (
            remote(
                part_send.at[j, rows, :],
                part_recv.at[j, rows, :],
                swap_send.at[0],
                swap_recv.at[0, j, piece],
                mirror_dev,
            ),
            remote(
                stat_send.at[j, :, rows],
                stat_recv.at[j, :, rows],
                swap_send.at[1],
                swap_recv.at[1, j, piece],
                mirror_dev,
            ),
        )

    def spread(half, j, piece):
        place = gathered.at[half * chunks + j, pl.ds(piece * piece_rows, piece_rows), :]
        return [
            remote(
                place,
                place,
                gather_send.at[way],
                gather_recv.at[half * chunks + j, piece],
                device,
            )
            for way, device in enumerate((side_dev, mate_dev))
        ]

    def block_rows(block):
        return pl.ds(pl.multiple_of(block * BLK, BLK), BLK)

    gate_copy = pltpu.make_async_copy(gate_in, gate, gate_sem)
    unit = math.log2(math.e) / math.sqrt(HD)

    def prepare_bias():
        live = blocks_ref[0] * BLK
        positions = camp * camp_history + lax.broadcasted_iota(
            jnp.int32, (1, camp_history), 1
        )
        history_bias = jnp.where(positions < live, 0.0, NEGATIVE)
        for block in range(block_count):
            bias[block : block + 1, 0:camp_history] = history_bias
            for part in range(2):
                for near in range(camp_blocks):
                    column = part * block_count + camp * camp_blocks + near
                    shown = jnp.full((1, BLK), mask_ref[0, block, column], jnp.int32)
                    begin = camp_history + part * camp_rows + near * BLK
                    bias[block : block + 1, begin : begin + BLK] = jnp.where(
                        shown > 0, 0.0, NEGATIVE
                    )

    def attend(j, piece):
        rows = pl.ds(piece * piece_rows, piece_rows)
        scores = lax.dot_general(
            queries[j, rows, :],
            kv[j, 0],
            (((1,), (1,)), ((), ())),
            preferred_element_type=jnp.float32,
        )
        peaks, sums, parts = [], [], []
        for place in range(piece_blocks):
            block = piece * piece_blocks + place
            part = scores[place * BLK : (place + 1) * BLK] * unit + bias[block : block + 1, :]
            peak = jnp.max(part, axis=1, keepdims=True)
            part = jnp.exp2(part - peak)
            peaks.append(peak)
            sums.append(jnp.sum(part, axis=1, keepdims=True))
            parts.append(part.astype(jnp.bfloat16))
        output = jnp.dot(
            jnp.concatenate(parts, axis=0), kv[j, 1], preferred_element_type=jnp.float32
        )
        output = output / jnp.concatenate(sums, axis=0)
        own_part[j, rows, :] = output
        part_send[j, rows, :] = output.astype(jnp.bfloat16)
        for place in range(piece_blocks):
            begin = piece * piece_rows + place * BLK
            level = jnp.broadcast_to(peaks[place] + jnp.log2(sums[place]), (BLK, BLK))
            own_lse[j, begin : begin + BLK, :] = level
            stat_send[j, :, begin : begin + BLK] = level.T[0:8, :]

    def combine(j, piece):
        def step(block, carry):
            rows = block_rows(block)
            mine = own_lse[j, rows, :]
            theirs = jnp.broadcast_to(stat_recv[j, 0:1, rows], (BLK, BLK)).T
            top = jnp.maximum(mine, theirs)
            first = jnp.exp2(mine - top)
            second = jnp.exp2(theirs - top)
            mixed = own_part[j, rows, :] * first + part_recv[j, rows, :].astype(
                jnp.float32
            ) * second
            gathered[col * chunks + j, rows, :] = (mixed / (first + second)).astype(
                jnp.bfloat16
            )
            return carry

        lax.fori_loop(piece * piece_blocks, (piece + 1) * piece_blocks, step, 0)

    def project(j, halves, last):
        for piece in range(PIECES):
            for half in halves:
                spread(half, j, piece)[0].wait_recv()

            def step(block, carry):
                rows = block_rows(block)
                left = jnp.concatenate(
                    [gathered[j, rows, :], gathered[chunks + j, rows, :]], axis=1
                )
                right = jnp.concatenate([weight[0, j], weight[1, j]], axis=0)
                part = jnp.dot(left, right, preferred_element_type=jnp.float32)
                part = part + total[rows, :]
                if last:
                    factor = gate[pl.ds(level_ref[0], 1), :]
                    out_ref[0, rows, :] = (part * factor).astype(out_ref.dtype)
                else:
                    total[rows, :] = part
                return carry

            lax.fori_loop(piece * piece_blocks, (piece + 1) * piece_blocks, step, 0)

    def every(body, count=chunks, first=0):
        def step(j, carry):
            body(j)
            return carry

        lax.fori_loop(first, count, step, 0)

    def start(copies):
        for copy in copies:
            copy.start()

    weight_copy = pltpu.make_async_copy(weight_in, weight, weight_sem)
    scalar_copies = [
        pltpu.make_async_copy(source, target, scalar_sem.at[place])
        for place, (source, target) in enumerate(
            ((mask_in, mask_ref), (blocks_in, blocks_ref), (level_in, level_ref))
        )
    ]
    own_half = gathered.at[pl.ds(pl.multiple_of(col * chunks, chunks), chunks)]

    def await_own(slot):
        await_bytes(kv.at[:, 0, 0:history_rows, :], in_send.at[0, slot])
        await_bytes(kv.at[:, :, 0:local_rows, :], in_send.at[1, slot])
        await_bytes(queries.at[:, 0:local_rows, :], in_send.at[2, slot])

    @pl.when(inner)
    def _():
        def ask(j):
            start(own_copies(1 - col, j, side_dev, 0, seat, ASKED))

        def begin(j):
            start(own_copies(1 - col, j, side_dev, 0, seat, ROWS))
            pl.when(j + EARLY < chunks)(lambda: ask(j + EARLY))

        every(ask, EARLY)
        every(begin, SIDE_AHEAD)
        start(scalar_copies)
        every(lambda j: start(local_copies(j)))
        weight_copy.start()
        gate_copy.start()
        total[...] = jnp.zeros_like(total)
        for copy in scalar_copies:
            copy.wait()
        prepare_bias()

        def answer(j):
            await_bytes(wholes(j)[2], in_recv.at[2, j])
            mirrored_query(j, camp_span).start()

        every(answer, EARLY)

        def take(j):
            await_bytes(wholes(j)[0], in_recv.at[0, j])
            passed_history(j, core).start()
            await_bytes(wholes(j)[1], in_recv.at[1, j])
            passed_fresh(j).start()
            pl.when(j + SIDE_AHEAD < chunks)(lambda: begin(j + SIDE_AHEAD))
            pl.when(j + EARLY < chunks)(lambda: answer(j + EARLY))

        def work(j):
            mirrored_query(j, far_span).wait_recv()
            passed_history(j, 1 - core).wait_recv()
            passed_fresh(j).wait_recv()
            for piece in range(PIECES):
                attend(j, piece)
                start(swapped(j, piece))

        def merge(j):
            for piece in range(PIECES):
                for copy in swapped(j, piece):
                    copy.wait_recv()
                combine(j, piece)
                start(spread(col, j, piece))

        def round_of(step):
            pl.when(step == INNER_LAG)(weight_copy.wait)
            pl.when(step < chunks)(lambda: take(step))
            pl.when((step >= COMBINE_LAG) & (step < chunks + COMBINE_LAG))(
                lambda: merge(step - COMBINE_LAG)
            )
            pl.when(step >= INNER_LAG)(
                lambda: project(step - INNER_LAG, (1 - col,), False)
            )
            pl.when(step < chunks)(lambda: work(step))

        every(round_of, chunks - 1 + INNER_LAG)
        gate_copy.wait()
        project(chunks - 1, (1 - col,), True)
        await_own(0)
        await_bytes(kv.at[:, 0, 0:camp_history, :], pass_send.at[0])
        await_bytes(kv.at[:, :, 0:camp_rows, :], pass_send.at[1])
        await_bytes(queries.at[:, 0:camp_rows, :], query_send)
        await_bytes(part_send, swap_send.at[0])
        await_bytes(stat_send, swap_send.at[1])
        await_bytes(own_half, gather_send.at[0])
        await_bytes(own_half, gather_send.at[1])

    @pl.when(jnp.logical_not(inner))
    def _():
        def ask(j):
            start(own_copies(1 - col, j, side_dev, 1, seat, ASKED))
            start(own_copies(col, j, mate_dev, 0, seat, ASKED))

        def begin(j):
            start(own_copies(col, j, mate_dev, 0, seat, ROWS))

        def begin_side(j):
            start(own_copies(1 - col, j, side_dev, 1, seat, ROWS))
            pl.when(j + EARLY < chunks)(lambda: ask(j + EARLY))

        every(ask, EARLY)
        every(begin, AHEAD)
        every(begin_side, SIDE_AHEAD)
        scalar_copies[2].start()
        weight_copy.start()
        gate_copy.start()
        total[...] = jnp.zeros_like(total)

        def pass_on(j, kinds):
            arrivals = own_copies(col, j, side_dev, 1, side_seat, kinds)
            copies = forward(j, kinds)
            for arrival, copy in zip(arrivals, copies):
                arrival.wait_recv()
                copy.start()

        every(lambda j: pass_on(j, ASKED), EARLY)

        def hand_on(j):
            pass_on(j, ROWS)
            pl.when(j + AHEAD < chunks)(lambda: begin(j + AHEAD))
            pl.when(j + SIDE_AHEAD < chunks)(lambda: begin_side(j + SIDE_AHEAD))
            pl.when(j + EARLY < chunks)(lambda: pass_on(j + EARLY, ASKED))

        def settle(j):
            for copy in forward(j, ROWS + ASKED):
                copy.wait_send()

        def relay(j):
            for piece in range(PIECES):
                copy = spread(col, j, piece)[0]
                copy.wait_recv()
                copy.start()

        def round_of(step):
            pl.when(step == OUTER_LAG)(weight_copy.wait)
            pl.when(step < chunks)(lambda: hand_on(step))
            pl.when((step >= THROTTLE) & (step < chunks + THROTTLE))(
                lambda: settle(step - THROTTLE)
            )
            pl.when((step >= RELAY_LAG) & (step < chunks + RELAY_LAG))(
                lambda: relay(step - RELAY_LAG)
            )
            pl.when(step >= OUTER_LAG)(
                lambda: project(step - OUTER_LAG, (1 - col,), False)
            )

        every(round_of, chunks - 1 + OUTER_LAG)
        gate_copy.wait()
        scalar_copies[2].wait()
        project(chunks - 1, (1 - col,), True)
        await_own(0)
        await_own(1)
        await_bytes(own_half, gather_send.at[0])


def on_device_fused(
    query, stretch_kv, history_kv, block_mask, noise_level, history_blocks, out_weight, gate_table
):
    n = lax.axis_size("tp")
    chunks = H // 2
    local_rows, history_rows = query.shape[1], history_kv.shape[1]
    row_count = n * local_rows
    key_count = (n * history_rows + 2 * row_count) // 2
    wide = out_weight.shape[1]
    block_count = block_mask.shape[1]
    anywhere = pl.BlockSpec(memory_space=pl.ANY)
    vector = pl.BlockSpec(memory_space=pltpu.VMEM)
    dma = pltpu.SemaphoreType.DMA
    return pl.pallas_call(
        functools.partial(fused_kernel, n, chunks),
        out_shape=jax.ShapeDtypeStruct((1, row_count, wide), jnp.bfloat16),
        in_specs=[anywhere] * 8,
        out_specs=vector,
        scratch_shapes=[
            pltpu.VMEM((chunks, 2, key_count, HD), jnp.bfloat16),
            pltpu.VMEM((chunks, row_count, HD), jnp.bfloat16),
            pltpu.VMEM((chunks, row_count, HD), jnp.float32),
            pltpu.VMEM((chunks, row_count, HD), jnp.float32),
            pltpu.VMEM((chunks, row_count, HD), jnp.bfloat16),
            pltpu.VMEM((chunks, row_count, HD), jnp.bfloat16),
            pltpu.VMEM((chunks, 8, row_count), jnp.float32),
            pltpu.VMEM((chunks, 8, row_count), jnp.float32),
            pltpu.VMEM((2 * chunks, row_count, HD), jnp.bfloat16),
            pltpu.VMEM((2, chunks, HD, wide), jnp.bfloat16),
            pltpu.VMEM(gate_table.shape, jnp.float32),
            pltpu.VMEM((block_count, key_count), jnp.float32),
            pltpu.VMEM((row_count, wide), jnp.float32),
            pltpu.SMEM(block_mask.shape, jnp.int32),
            pltpu.SMEM(history_blocks.shape, jnp.int32),
            pltpu.SMEM(noise_level.shape, jnp.int32),
            dma((3, 2)),
            dma((3, chunks)),
            dma((3, chunks)),
            dma((2,)),
            dma((2, chunks)),
            dma,
            dma((chunks,)),
            dma((2,)),
            dma((2, chunks, PIECES)),
            dma((2,)),
            dma((2 * chunks, PIECES)),
            dma,
            dma,
            dma((3,)),
        ],
        compiler_params=pltpu.CompilerParams(
            collective_id=0, has_side_effects=True, vmem_limit_bytes=63 * 1024 * 1024
        ),
    )(
        block_mask,
        history_blocks,
        noise_level,
        query,
        stretch_kv,
        history_kv,
        out_weight.reshape(2, chunks, HD, wide),
        gate_table,
    )


def solution(mesh):
    count = mesh.shape["tp"]
    fits = H % 2 == 0 and count // 2 == 4 and count % 2 == 0 and mesh.shape["stretch"] == 2
    return jax.shard_map(
        on_device_fused if fits else on_device,
        mesh=mesh,
        in_specs=(
            P(("rep", "stretch"), "tp", None),
            P(None, ("rep", "stretch"), "tp", None),
            P(None, ("rep", "tp"), None),
            P(("rep", "stretch"), None, None),
            P(("rep", "stretch")),
            P("rep"),
            P(None, "tp"),
            P(None, "tp"),
        ),
        out_specs=P(("rep", "stretch"), None, "tp"),
        check_vma=False,
    )
```

```python
import functools
import math

import jax
import jax.numpy as jnp
from jax import lax
from jax.experimental import pallas as pl
from jax.experimental.pallas import tpu as pltpu
from jax.sharding import PartitionSpec as P

H = 24
HD = 128
BLK = 128


NEGATIVE = -1e30


def shifted(value, axis, steps):
    count = lax.axis_size(axis)
    first, last = (max(0, -steps), min(count, count - steps))
    return lax.ppermute(value, axis, [(source, source + steps) for source in range(first, last)])


def head_block(queries, key_rows, value_rows, allowed):
    key_count = key_rows.shape[0]
    head_count = queries.shape[1]
    key_heads = key_rows.reshape(key_count, head_count, HD)
    scores = jnp.einsum("qhd,khd->qhk", queries, key_heads, preferred_element_type=jnp.float32) * (
        1.0 / math.sqrt(HD)
    )
    scores = jnp.where(allowed[:, None, :], scores, NEGATIVE)
    row_peak = jnp.max(scores, axis=2)
    weights = jnp.where(allowed[:, None, :], jnp.exp(scores - row_peak[:, :, None]), 0.0)
    weight_sum = jnp.sum(weights, axis=2)
    output = None
    value_heads = value_rows.reshape(key_count, head_count, HD).astype(jnp.float32)
    output = jnp.einsum("qhk,khd->qhd", weights, value_heads, precision=lax.Precision.HIGHEST)
    return (row_peak, weight_sum, output)


def combine(earlier, later):
    row_peak = jnp.maximum(earlier[0], later[0])
    scale_one = jnp.exp(earlier[0] - row_peak)
    scale_two = jnp.exp(later[0] - row_peak)
    weight_sum = earlier[1] * scale_one + later[1] * scale_two
    output = None
    output = earlier[2] * scale_one[:, :, None] + later[2] * scale_two[:, :, None]
    return (row_peak, weight_sum, output)


def column_table(columns, block_count):
    return (columns[:, None] == jnp.arange(2 * block_count, dtype=jnp.int32)[None, :]).astype(
        jnp.float32
    )


def attend_all(
    queries,
    query_positions,
    fresh_keys,
    fresh_values,
    fresh_hot,
    mask_table,
    history_pair,
    history_live,
    span,
):
    row_count = queries.shape[0]
    head_count = queries.shape[1]
    block_count = mask_table.shape[0]
    query_hot = (
        (query_positions // BLK)[:, None] == jnp.arange(block_count, dtype=jnp.int32)[None, :]
    ).astype(jnp.float32)
    fresh_allowed = jnp.dot(jnp.dot(query_hot, mask_table), fresh_hot.T) > 0.5
    base_peak = jnp.full((row_count, head_count), NEGATIVE, jnp.float32)
    skipped = (
        base_peak,
        jnp.zeros((row_count, head_count), jnp.float32),
        jnp.zeros((row_count, head_count, HD), jnp.float32),
    )
    result = head_block(queries, fresh_keys, fresh_values, fresh_allowed)
    for sub_block in range(history_pair.shape[1] // span):
        lower_row = sub_block * span
        key_rows = history_pair[0, lower_row : lower_row + span]
        value_rows = history_pair[1, lower_row : lower_row + span]
        live_rows = history_live[lower_row : lower_row + span]
        allowed = jnp.broadcast_to(live_rows[None, :], (row_count, span))
        block_part = lax.cond(
            jnp.any(live_rows),
            lambda: head_block(queries, key_rows, value_rows, allowed),
            lambda: skipped,
        )
        result = combine(result, block_part)
    return result


def on_device(
    query, stretch_kv, history_kv, block_mask, noise_level, history_blocks, out_weight, gate_table
):
    tp_count = lax.axis_size("tp")
    tp_index = lax.axis_index("tp")
    local_rows = query.shape[1]
    feature_width = query.shape[2]
    history_rows = history_kv.shape[1]
    block_count = block_mask.shape[1]
    own_pair = stretch_kv[:, 0]
    older_pair = shifted(own_pair, "stretch", 1)
    mask_table = block_mask[0].astype(jnp.float32)
    live_limit = history_blocks[0] * BLK
    fresh_keys = jnp.concatenate([older_pair[0], own_pair[0]], 0)
    fresh_values = jnp.concatenate([older_pair[1], own_pair[1]], 0)
    own_positions = tp_index * local_rows + jnp.arange(local_rows, dtype=jnp.int32)
    fresh_hot = column_table(
        jnp.concatenate([own_positions // BLK, block_count + own_positions // BLK], 0), block_count
    )
    history_positions = tp_index * history_rows + jnp.arange(history_rows, dtype=jnp.int32)
    history_live = history_positions < live_limit
    piece = lax.all_gather(query[0], "tp", axis=0, tiled=True)
    row_count = piece.shape[0]
    positions = jnp.arange(row_count, dtype=jnp.int32)
    row_peak, weight_sum, output = attend_all(
        piece.reshape(row_count, H, HD),
        positions,
        fresh_keys,
        fresh_values,
        fresh_hot,
        mask_table,
        history_kv,
        history_live,
        BLK,
    )
    got_outputs, got_peaks, got_sums = (
        lax.all_to_all(
            output.reshape(tp_count, local_rows, H, HD),
            "tp",
            split_axis=0,
            concat_axis=0,
            tiled=True,
        ),
        lax.all_to_all(
            row_peak.reshape(tp_count, local_rows, H), "tp", split_axis=0, concat_axis=0, tiled=True
        ),
        lax.all_to_all(
            weight_sum.reshape(tp_count, local_rows, H),
            "tp",
            split_axis=0,
            concat_axis=0,
            tiled=True,
        ),
    )
    overall = jnp.max(got_peaks, axis=0)
    factor = jnp.exp(got_peaks - overall[None])
    merged_sum = jnp.sum(got_sums * factor, axis=0)
    merged = jnp.sum(got_outputs * factor[:, :, :, None], axis=0) / merged_sum[:, :, None]
    attended = merged.reshape(local_rows, feature_width).astype(jnp.bfloat16)
    projected = jnp.dot(
        lax.all_gather(attended, "tp", axis=0, tiled=True),
        out_weight,
        preferred_element_type=jnp.float32,
    )
    level_hot = (jnp.arange(gate_table.shape[0], dtype=jnp.int32) == noise_level[0]).astype(
        jnp.float32
    )[None, :]
    gate_row = jnp.dot(level_hot, gate_table, precision=lax.Precision.HIGHEST)
    return (projected * gate_row).astype(jnp.bfloat16)[None]


MESH = pl.DeviceIdType.MESH
ROWS = (0, 1)
ASKED = (2,)
PIECES = 2
AHEAD = 1
SIDE_AHEAD = 6
THROTTLE = 2
EARLY = 5
COMBINE_LAG = 2
INNER_LAG = 5
RELAY_LAG = 5
OUTER_LAG = 8


def fused_kernel(
    n,
    chunks,
    mask_in,
    blocks_in,
    level_in,
    query_in,
    fresh_in,
    history_in,
    weight_in,
    gate_in,
    out_ref,
    kv,
    queries,
    own_part,
    own_lse,
    part_send,
    part_recv,
    stat_send,
    stat_recv,
    gathered,
    weight,
    gate,
    bias,
    total,
    mask_ref,
    blocks_ref,
    level_ref,
    in_send,
    in_recv,
    forward_send,
    pass_send,
    pass_recv,
    query_send,
    query_recv,
    swap_send,
    swap_recv,
    gather_send,
    gather_recv,
    weight_sem,
    gate_sem,
    scalar_sem,
):
    me = lax.axis_index("tp")
    core = lax.axis_index("stretch")
    twin = {"stretch": 1 - core}
    line = n // 2
    spot, col = me // 2, me % 2
    members = n // 2
    camp = me // members
    seat = me % members
    inner = (spot > 0) & (spot < line - 1)
    mate_spot = spot + 1 - 2 * (spot % 2)
    side_dev = {"tp": me + 1 - 2 * col}
    mate_dev = {"tp": 2 * mate_spot + col}
    mirror_dev = {"tp": 2 * (line - 1 - spot) + col}
    side_seat = seat + 1 - 2 * col

    local_rows = query_in.shape[1]
    history_rows = history_in.shape[1]
    row_count = n * local_rows
    camp_rows = members * local_rows
    camp_history = members * history_rows
    other_base = camp_history
    own_base = camp_history + camp_rows
    block_count = mask_in.shape[1]
    camp_blocks = block_count // 2
    piece_blocks = block_count // PIECES
    piece_rows = piece_blocks * BLK
    wide = out_ref.shape[2]

    barrier = pltpu.get_barrier_semaphore()

    def greet(devices):
        for device in devices:
            pl.semaphore_signal(barrier, inc=1, device_id=device, device_id_type=MESH)

    greet((side_dev, mate_dev))
    pl.when(inner)(lambda: greet((mirror_dev, twin)))
    pl.semaphore_wait(barrier, jnp.where(inner, 4, 2))

    def remote(source, target, send, recv, device):
        return pltpu.make_async_remote_copy(
            src_ref=source,
            dst_ref=target,
            send_sem=send,
            recv_sem=recv,
            device_id=device,
            device_id_type=MESH,
        )

    def columns(half, j):
        return pl.ds(pl.multiple_of((half * chunks + j) * HD, HD), HD)

    def history_span(source):
        return pl.ds(pl.multiple_of(source * history_rows, history_rows), history_rows)

    def fresh_span(base, source):
        return pl.ds(pl.multiple_of(base + source * local_rows, local_rows), local_rows)

    def query_span(source):
        return pl.ds(
            pl.multiple_of((camp * members + source) * local_rows, local_rows), local_rows
        )

    camp_span = pl.ds(pl.multiple_of(camp * camp_rows, camp_rows), camp_rows)
    far_span = pl.ds(pl.multiple_of((1 - camp) * camp_rows, camp_rows), camp_rows)

    def places(j, source):
        return (
            kv.at[j, core, history_span(source), :],
            kv.at[j, :, fresh_span(own_base, source), :],
            queries.at[j, query_span(source), :],
        )

    def wholes(j):
        return (
            kv.at[j, core, 0:camp_history, :],
            kv.at[j, :, own_base : own_base + camp_rows, :],
            queries.at[j, camp_span, :],
        )

    def origins(half, j):
        cols = columns(half, j)
        return (
            history_in.at[core, :, cols],
            fresh_in.at[:, 0, :, cols],
            query_in.at[0, :, cols],
        )

    def own_copies(half, j, device, slot, source, kinds):
        from_refs, to_refs = origins(half, j), places(j, source)
        return [
            remote(from_refs[k], to_refs[k], in_send.at[k, slot], in_recv.at[k, j], device)
            for k in kinds
        ]

    def forward(j, kinds):
        spots = places(j, side_seat)
        return [
            remote(spots[k], spots[k], forward_send.at[k, j], in_recv.at[k, j], mate_dev)
            for k in kinds
        ]

    def local_copies(j):
        from_refs, to_refs = origins(col, j), places(j, seat)
        return [
            pltpu.make_async_copy(from_refs[k], to_refs[k], in_recv.at[k, j]) for k in range(3)
        ]

    def await_bytes(ref, sem):
        pltpu.make_async_copy(ref, ref, sem).wait()

    def passed_history(j, which):
        place = kv.at[j, which, 0:camp_history, :]
        return remote(place, place, pass_send.at[0], pass_recv.at[0, j], twin)

    def passed_fresh(j):
        return remote(
            kv.at[j, :, own_base : own_base + camp_rows, :],
            kv.at[j, :, other_base : other_base + camp_rows, :],
            pass_send.at[1],
            pass_recv.at[1, j],
            twin,
        )

    def mirrored_query(j, span):
        place = queries.at[j, span, :]
        return remote(place, place, query_send, query_recv.at[j], mirror_dev)

    def swapped(j, piece):
        rows = pl.ds(piece * piece_rows, piece_rows)
        return (
            remote(
                part_send.at[j, rows, :],
                part_recv.at[j, rows, :],
                swap_send.at[0],
                swap_recv.at[0, j, piece],
                mirror_dev,
            ),
            remote(
                stat_send.at[j, :, rows],
                stat_recv.at[j, :, rows],
                swap_send.at[1],
                swap_recv.at[1, j, piece],
                mirror_dev,
            ),
        )

    def spread(half, j, piece):
        place = gathered.at[half * chunks + j, pl.ds(piece * piece_rows, piece_rows), :]
        return [
            remote(
                place,
                place,
                gather_send.at[way],
                gather_recv.at[half * chunks + j, piece],
                device,
            )
            for way, device in enumerate((side_dev, mate_dev))
        ]

    def block_rows(block):
        return pl.ds(pl.multiple_of(block * BLK, BLK), BLK)

    gate_copy = pltpu.make_async_copy(gate_in, gate, gate_sem)
    unit = math.log2(math.e) / math.sqrt(HD)

    def prepare_bias():
        live = blocks_ref[0] * BLK
        positions = camp * camp_history + lax.broadcasted_iota(
            jnp.int32, (1, camp_history), 1
        )
        history_bias = jnp.where(positions < live, 0.0, NEGATIVE)
        for block in range(block_count):
            bias[block : block + 1, 0:camp_history] = history_bias
            for part in range(2):
                for near in range(camp_blocks):
                    column = part * block_count + camp * camp_blocks + near
                    shown = jnp.full((1, BLK), mask_ref[0, block, column], jnp.int32)
                    begin = camp_history + part * camp_rows + near * BLK
                    bias[block : block + 1, begin : begin + BLK] = jnp.where(
                        shown > 0, 0.0, NEGATIVE
                    )

    def attend(j, piece):
        rows = pl.ds(piece * piece_rows, piece_rows)
        scores = lax.dot_general(
            queries[j, rows, :],
            kv[j, 0],
            (((1,), (1,)), ((), ())),
            preferred_element_type=jnp.float32,
        )
        peaks, sums, parts = [], [], []
        for place in range(piece_blocks):
            block = piece * piece_blocks + place
            part = scores[place * BLK : (place + 1) * BLK] * unit + bias[block : block + 1, :]
            peak = jnp.max(part, axis=1, keepdims=True)
            part = jnp.exp2(part - peak)
            peaks.append(peak)
            sums.append(jnp.sum(part, axis=1, keepdims=True))
            parts.append(part.astype(jnp.bfloat16))
        output = jnp.dot(
            jnp.concatenate(parts, axis=0), kv[j, 1], preferred_element_type=jnp.float32
        )
        output = output / jnp.concatenate(sums, axis=0)
        own_part[j, rows, :] = output
        part_send[j, rows, :] = output.astype(jnp.bfloat16)
        for place in range(piece_blocks):
            begin = piece * piece_rows + place * BLK
            level = jnp.broadcast_to(peaks[place] + jnp.log2(sums[place]), (BLK, BLK))
            own_lse[j, begin : begin + BLK, :] = level
            stat_send[j, :, begin : begin + BLK] = level.T[0:8, :]

    def combine(j, piece):
        def step(block, carry):
            rows = block_rows(block)
            mine = own_lse[j, rows, :]
            theirs = jnp.broadcast_to(stat_recv[j, 0:1, rows], (BLK, BLK)).T
            top = jnp.maximum(mine, theirs)
            first = jnp.exp2(mine - top)
            second = jnp.exp2(theirs - top)
            mixed = own_part[j, rows, :] * first + part_recv[j, rows, :].astype(
                jnp.float32
            ) * second
            gathered[col * chunks + j, rows, :] = (mixed / (first + second)).astype(
                jnp.bfloat16
            )
            return carry

        lax.fori_loop(piece * piece_blocks, (piece + 1) * piece_blocks, step, 0)

    def project(j, halves, last):
        for piece in range(PIECES):
            for half in halves:
                spread(half, j, piece)[0].wait_recv()

            def step(block, carry):
                rows = block_rows(block)
                left = jnp.concatenate(
                    [gathered[j, rows, :], gathered[chunks + j, rows, :]], axis=1
                )
                right = jnp.concatenate([weight[0, j], weight[1, j]], axis=0)
                part = jnp.dot(left, right, preferred_element_type=jnp.float32)
                part = part + total[rows, :]
                if last:
                    factor = gate[pl.ds(level_ref[0], 1), :]
                    out_ref[0, rows, :] = (part * factor).astype(out_ref.dtype)
                else:
                    total[rows, :] = part
                return carry

            lax.fori_loop(piece * piece_blocks, (piece + 1) * piece_blocks, step, 0)

    def every(body, count=chunks, first=0):
        def step(j, carry):
            body(j)
            return carry

        lax.fori_loop(first, count, step, 0)

    def start(copies):
        for copy in copies:
            copy.start()

    weight_copy = pltpu.make_async_copy(weight_in, weight, weight_sem)
    scalar_copies = [
        pltpu.make_async_copy(source, target, scalar_sem.at[place])
        for place, (source, target) in enumerate(
            ((mask_in, mask_ref), (blocks_in, blocks_ref), (level_in, level_ref))
        )
    ]
    own_half = gathered.at[pl.ds(pl.multiple_of(col * chunks, chunks), chunks)]

    def await_own(slot):
        await_bytes(kv.at[:, 0, 0:history_rows, :], in_send.at[0, slot])
        await_bytes(kv.at[:, :, 0:local_rows, :], in_send.at[1, slot])
        await_bytes(queries.at[:, 0:local_rows, :], in_send.at[2, slot])

    @pl.when(inner)
    def _():
        def ask(j):
            start(own_copies(1 - col, j, side_dev, 0, seat, ASKED))

        def begin(j):
            start(own_copies(1 - col, j, side_dev, 0, seat, ROWS))
            pl.when(j + EARLY < chunks)(lambda: ask(j + EARLY))

        start(own_copies(1 - col, 0, side_dev, 0, seat, ROWS))
        every(ask, EARLY + 1)
        every(begin, SIDE_AHEAD, 1)
        start(scalar_copies)
        every(lambda j: start(local_copies(j)))
        weight_copy.start()
        gate_copy.start()
        total[...] = jnp.zeros_like(total)
        for copy in scalar_copies:
            copy.wait()
        prepare_bias()

        def answer(j):
            await_bytes(wholes(j)[2], in_recv.at[2, j])
            mirrored_query(j, camp_span).start()

        every(answer, EARLY)

        def take(j):
            await_bytes(wholes(j)[0], in_recv.at[0, j])
            passed_history(j, core).start()
            await_bytes(wholes(j)[1], in_recv.at[1, j])
            passed_fresh(j).start()
            pl.when(j + SIDE_AHEAD < chunks)(lambda: begin(j + SIDE_AHEAD))
            pl.when(j + EARLY < chunks)(lambda: answer(j + EARLY))

        def work(j):
            mirrored_query(j, far_span).wait_recv()
            passed_history(j, 1 - core).wait_recv()
            passed_fresh(j).wait_recv()
            for piece in range(PIECES):
                attend(j, piece)
                start(swapped(j, piece))

        def merge(j):
            for piece in range(PIECES):
                for copy in swapped(j, piece):
                    copy.wait_recv()
                combine(j, piece)
                start(spread(col, j, piece))

        def round_of(step):
            pl.when(step == INNER_LAG)(weight_copy.wait)
            pl.when(step < chunks)(lambda: take(step))
            pl.when((step >= COMBINE_LAG) & (step < chunks + COMBINE_LAG))(
                lambda: merge(step - COMBINE_LAG)
            )
            pl.when(step >= INNER_LAG)(
                lambda: project(step - INNER_LAG, (1 - col,), False)
            )
            pl.when(step < chunks)(lambda: work(step))

        every(round_of, chunks - 1 + INNER_LAG)
        gate_copy.wait()
        project(chunks - 1, (1 - col,), True)
        await_own(0)
        await_bytes(kv.at[:, 0, 0:camp_history, :], pass_send.at[0])
        await_bytes(kv.at[:, :, 0:camp_rows, :], pass_send.at[1])
        await_bytes(queries.at[:, 0:camp_rows, :], query_send)
        await_bytes(part_send, swap_send.at[0])
        await_bytes(stat_send, swap_send.at[1])
        await_bytes(own_half, gather_send.at[0])
        await_bytes(own_half, gather_send.at[1])

    @pl.when(jnp.logical_not(inner))
    def _():
        def ask(j):
            start(own_copies(1 - col, j, side_dev, 1, seat, ASKED))
            start(own_copies(col, j, mate_dev, 0, seat, ASKED))

        def begin(j):
            start(own_copies(col, j, mate_dev, 0, seat, ROWS))

        def begin_side(j):
            start(own_copies(1 - col, j, side_dev, 1, seat, ROWS))
            pl.when(j + EARLY < chunks)(lambda: ask(j + EARLY))

        start(own_copies(1 - col, 0, side_dev, 1, seat, ROWS))
        begin(0)
        every(ask, EARLY + 1)
        every(begin, AHEAD, 1)
        every(begin_side, SIDE_AHEAD, 1)
        scalar_copies[2].start()
        weight_copy.start()
        gate_copy.start()
        total[...] = jnp.zeros_like(total)

        def pass_on(j, kinds):
            arrivals = own_copies(col, j, side_dev, 1, side_seat, kinds)
            copies = forward(j, kinds)
            for arrival, copy in zip(arrivals, copies):
                arrival.wait_recv()
                copy.start()

        every(lambda j: pass_on(j, ASKED), EARLY)

        def hand_on(j):
            pass_on(j, ROWS)
            pl.when(j + AHEAD < chunks)(lambda: begin(j + AHEAD))
            pl.when(j + SIDE_AHEAD < chunks)(lambda: begin_side(j + SIDE_AHEAD))
            pl.when(j + EARLY < chunks)(lambda: pass_on(j + EARLY, ASKED))

        def settle(j):
            for copy in forward(j, ROWS + ASKED):
                copy.wait_send()

        def relay(j):
            for piece in range(PIECES):
                copy = spread(col, j, piece)[0]
                copy.wait_recv()
                copy.start()

        def round_of(step):
            pl.when(step == OUTER_LAG)(weight_copy.wait)
            pl.when(step < chunks)(lambda: hand_on(step))
            pl.when((step >= THROTTLE) & (step < chunks + THROTTLE))(
                lambda: settle(step - THROTTLE)
            )
            pl.when((step >= RELAY_LAG) & (step < chunks + RELAY_LAG))(
                lambda: relay(step - RELAY_LAG)
            )
            pl.when(step >= OUTER_LAG)(
                lambda: project(step - OUTER_LAG, (1 - col,), False)
            )

        every(round_of, chunks - 1 + OUTER_LAG)
        gate_copy.wait()
        scalar_copies[2].wait()
        project(chunks - 1, (1 - col,), True)
        await_own(0)
        await_own(1)
        await_bytes(own_half, gather_send.at[0])


def on_device_fused(
    query, stretch_kv, history_kv, block_mask, noise_level, history_blocks, out_weight, gate_table
):
    n = lax.axis_size("tp")
    chunks = H // 2
    local_rows, history_rows = query.shape[1], history_kv.shape[1]
    row_count = n * local_rows
    key_count = (n * history_rows + 2 * row_count) // 2
    wide = out_weight.shape[1]
    block_count = block_mask.shape[1]
    vector = pl.BlockSpec(memory_space=pltpu.VMEM)
    dma = pltpu.SemaphoreType.DMA
    return pl.pallas_call(
        functools.partial(fused_kernel, n, chunks),
        out_shape=pltpu.VMEM((1, row_count, wide), jnp.bfloat16),
        in_specs=[pl.BlockSpec(memory_space=pltpu.HBM)] * 8,
        out_specs=vector,
        scratch_shapes=[
            pltpu.VMEM((chunks, 2, key_count, HD), jnp.bfloat16),
            pltpu.VMEM((chunks, row_count, HD), jnp.bfloat16),
            pltpu.VMEM((chunks, row_count, HD), jnp.float32),
            pltpu.VMEM((chunks, row_count, HD), jnp.float32),
            pltpu.VMEM((chunks, row_count, HD), jnp.bfloat16),
            pltpu.VMEM((chunks, row_count, HD), jnp.bfloat16),
            pltpu.VMEM((chunks, 8, row_count), jnp.float32),
            pltpu.VMEM((chunks, 8, row_count), jnp.float32),
            pltpu.VMEM((2 * chunks, row_count, HD), jnp.bfloat16),
            pltpu.VMEM((2, chunks, HD, wide), jnp.bfloat16),
            pltpu.VMEM(gate_table.shape, jnp.float32),
            pltpu.VMEM((block_count, key_count), jnp.float32),
            pltpu.VMEM((row_count, wide), jnp.float32),
            pltpu.SMEM(block_mask.shape, jnp.int32),
            pltpu.SMEM(history_blocks.shape, jnp.int32),
            pltpu.SMEM(noise_level.shape, jnp.int32),
            dma((3, 2)),
            dma((3, chunks)),
            dma((3, chunks)),
            dma((2,)),
            dma((2, chunks)),
            dma,
            dma((chunks,)),
            dma((2,)),
            dma((2, chunks, PIECES)),
            dma((2,)),
            dma((2 * chunks, PIECES)),
            dma,
            dma,
            dma((3,)),
        ],
        compiler_params=pltpu.CompilerParams(
            collective_id=0, has_side_effects=True, vmem_limit_bytes=63 * 1024 * 1024
        ),
    )(
        block_mask,
        history_blocks,
        noise_level,
        query,
        stretch_kv,
        history_kv,
        out_weight.reshape(2, chunks, HD, wide),
        gate_table,
    )


def solution(mesh):
    count = mesh.shape["tp"]
    fits = H % 2 == 0 and count // 2 == 4 and count % 2 == 0 and mesh.shape["stretch"] == 2
    return jax.shard_map(
        on_device_fused if fits else on_device,
        mesh=mesh,
        in_specs=(
            P(("rep", "stretch"), "tp", None),
            P(None, ("rep", "stretch"), "tp", None),
            P(None, ("rep", "tp"), None),
            P(("rep", "stretch"), None, None),
            P(("rep", "stretch")),
            P("rep"),
            P(None, "tp"),
            P(None, "tp"),
        ),
        out_specs=P(("rep", "stretch"), None, "tp"),
        check_vma=False,
    )
```

```python
import functools
import math

import jax
import jax.numpy as jnp
from jax import lax
from jax.experimental import pallas as pl
from jax.experimental.pallas import tpu as pltpu
from jax.sharding import PartitionSpec as P

H = 24
HD = 128
BLK = 128


NEGATIVE = -1e30


def shifted(value, axis, steps):
    count = lax.axis_size(axis)
    first, last = (max(0, -steps), min(count, count - steps))
    return lax.ppermute(value, axis, [(source, source + steps) for source in range(first, last)])


def head_block(queries, key_rows, value_rows, allowed):
    key_count = key_rows.shape[0]
    head_count = queries.shape[1]
    key_heads = key_rows.reshape(key_count, head_count, HD)
    scores = jnp.einsum("qhd,khd->qhk", queries, key_heads, preferred_element_type=jnp.float32) * (
        1.0 / math.sqrt(HD)
    )
    scores = jnp.where(allowed[:, None, :], scores, NEGATIVE)
    row_peak = jnp.max(scores, axis=2)
    weights = jnp.where(allowed[:, None, :], jnp.exp(scores - row_peak[:, :, None]), 0.0)
    weight_sum = jnp.sum(weights, axis=2)
    output = None
    value_heads = value_rows.reshape(key_count, head_count, HD).astype(jnp.float32)
    output = jnp.einsum("qhk,khd->qhd", weights, value_heads, precision=lax.Precision.HIGHEST)
    return (row_peak, weight_sum, output)


def combine(earlier, later):
    row_peak = jnp.maximum(earlier[0], later[0])
    scale_one = jnp.exp(earlier[0] - row_peak)
    scale_two = jnp.exp(later[0] - row_peak)
    weight_sum = earlier[1] * scale_one + later[1] * scale_two
    output = None
    output = earlier[2] * scale_one[:, :, None] + later[2] * scale_two[:, :, None]
    return (row_peak, weight_sum, output)


def column_table(columns, block_count):
    return (columns[:, None] == jnp.arange(2 * block_count, dtype=jnp.int32)[None, :]).astype(
        jnp.float32
    )


def attend_all(
    queries,
    query_positions,
    fresh_keys,
    fresh_values,
    fresh_hot,
    mask_table,
    history_pair,
    history_live,
    span,
):
    row_count = queries.shape[0]
    head_count = queries.shape[1]
    block_count = mask_table.shape[0]
    query_hot = (
        (query_positions // BLK)[:, None] == jnp.arange(block_count, dtype=jnp.int32)[None, :]
    ).astype(jnp.float32)
    fresh_allowed = jnp.dot(jnp.dot(query_hot, mask_table), fresh_hot.T) > 0.5
    base_peak = jnp.full((row_count, head_count), NEGATIVE, jnp.float32)
    skipped = (
        base_peak,
        jnp.zeros((row_count, head_count), jnp.float32),
        jnp.zeros((row_count, head_count, HD), jnp.float32),
    )
    result = head_block(queries, fresh_keys, fresh_values, fresh_allowed)
    for sub_block in range(history_pair.shape[1] // span):
        lower_row = sub_block * span
        key_rows = history_pair[0, lower_row : lower_row + span]
        value_rows = history_pair[1, lower_row : lower_row + span]
        live_rows = history_live[lower_row : lower_row + span]
        allowed = jnp.broadcast_to(live_rows[None, :], (row_count, span))
        block_part = lax.cond(
            jnp.any(live_rows),
            lambda: head_block(queries, key_rows, value_rows, allowed),
            lambda: skipped,
        )
        result = combine(result, block_part)
    return result


def on_device(
    query, stretch_kv, history_kv, block_mask, noise_level, history_blocks, out_weight, gate_table
):
    tp_count = lax.axis_size("tp")
    tp_index = lax.axis_index("tp")
    local_rows = query.shape[1]
    feature_width = query.shape[2]
    history_rows = history_kv.shape[1]
    block_count = block_mask.shape[1]
    own_pair = stretch_kv[:, 0]
    older_pair = shifted(own_pair, "stretch", 1)
    mask_table = block_mask[0].astype(jnp.float32)
    live_limit = history_blocks[0] * BLK
    fresh_keys = jnp.concatenate([older_pair[0], own_pair[0]], 0)
    fresh_values = jnp.concatenate([older_pair[1], own_pair[1]], 0)
    own_positions = tp_index * local_rows + jnp.arange(local_rows, dtype=jnp.int32)
    fresh_hot = column_table(
        jnp.concatenate([own_positions // BLK, block_count + own_positions // BLK], 0), block_count
    )
    history_positions = tp_index * history_rows + jnp.arange(history_rows, dtype=jnp.int32)
    history_live = history_positions < live_limit
    piece = lax.all_gather(query[0], "tp", axis=0, tiled=True)
    row_count = piece.shape[0]
    positions = jnp.arange(row_count, dtype=jnp.int32)
    row_peak, weight_sum, output = attend_all(
        piece.reshape(row_count, H, HD),
        positions,
        fresh_keys,
        fresh_values,
        fresh_hot,
        mask_table,
        history_kv,
        history_live,
        BLK,
    )
    got_outputs, got_peaks, got_sums = (
        lax.all_to_all(
            output.reshape(tp_count, local_rows, H, HD),
            "tp",
            split_axis=0,
            concat_axis=0,
            tiled=True,
        ),
        lax.all_to_all(
            row_peak.reshape(tp_count, local_rows, H), "tp", split_axis=0, concat_axis=0, tiled=True
        ),
        lax.all_to_all(
            weight_sum.reshape(tp_count, local_rows, H),
            "tp",
            split_axis=0,
            concat_axis=0,
            tiled=True,
        ),
    )
    overall = jnp.max(got_peaks, axis=0)
    factor = jnp.exp(got_peaks - overall[None])
    merged_sum = jnp.sum(got_sums * factor, axis=0)
    merged = jnp.sum(got_outputs * factor[:, :, :, None], axis=0) / merged_sum[:, :, None]
    attended = merged.reshape(local_rows, feature_width).astype(jnp.bfloat16)
    projected = jnp.dot(
        lax.all_gather(attended, "tp", axis=0, tiled=True),
        out_weight,
        preferred_element_type=jnp.float32,
    )
    level_hot = (jnp.arange(gate_table.shape[0], dtype=jnp.int32) == noise_level[0]).astype(
        jnp.float32
    )[None, :]
    gate_row = jnp.dot(level_hot, gate_table, precision=lax.Precision.HIGHEST)
    return (projected * gate_row).astype(jnp.bfloat16)[None]


MESH = pl.DeviceIdType.MESH
ROWS = (0, 1)
ASKED = (2,)
PIECES = 2
AHEAD = 1
SIDE_AHEAD = 6
THROTTLE = 2
EARLY = 5
COMBINE_LAG = 2
INNER_LAG = 5
RELAY_LAG = 5
OUTER_LAG = 8


def fused_kernel(
    n,
    chunks,
    mask_in,
    blocks_in,
    level_in,
    query_in,
    fresh_in,
    history_in,
    weight_in,
    gate_in,
    out_ref,
    kv,
    queries,
    own_part,
    own_lse,
    part_send,
    part_recv,
    stat_send,
    stat_recv,
    gathered,
    weight,
    gate,
    bias,
    total,
    mask_ref,
    blocks_ref,
    level_ref,
    in_send,
    in_recv,
    forward_send,
    pass_send,
    pass_recv,
    query_send,
    query_recv,
    swap_send,
    swap_recv,
    gather_send,
    gather_recv,
    weight_sem,
    gate_sem,
    scalar_sem,
):
    me = lax.axis_index("tp")
    core = lax.axis_index("stretch")
    twin = {"stretch": 1 - core}
    line = n // 2
    spot, col = me // 2, me % 2
    members = n // 2
    camp = me // members
    seat = me % members
    inner = (spot > 0) & (spot < line - 1)
    mate_spot = spot + 1 - 2 * (spot % 2)
    side_dev = {"tp": me + 1 - 2 * col}
    mate_dev = {"tp": 2 * mate_spot + col}
    mirror_dev = {"tp": 2 * (line - 1 - spot) + col}
    side_seat = seat + 1 - 2 * col

    local_rows = query_in.shape[1]
    history_rows = history_in.shape[1]
    row_count = n * local_rows
    camp_rows = members * local_rows
    camp_history = members * history_rows
    other_base = camp_history
    own_base = camp_history + camp_rows
    block_count = mask_in.shape[1]
    camp_blocks = block_count // 2
    piece_blocks = block_count // PIECES
    piece_rows = piece_blocks * BLK
    wide = out_ref.shape[2]

    barrier = pltpu.get_barrier_semaphore()

    def greet(devices):
        for device in devices:
            pl.semaphore_signal(barrier, inc=1, device_id=device, device_id_type=MESH)

    greet((side_dev, mate_dev))
    pl.when(inner)(lambda: greet((mirror_dev, twin)))
    pl.semaphore_wait(barrier, jnp.where(inner, 4, 2))

    def remote(source, target, send, recv, device):
        return pltpu.make_async_remote_copy(
            src_ref=source,
            dst_ref=target,
            send_sem=send,
            recv_sem=recv,
            device_id=device,
            device_id_type=MESH,
        )

    def columns(half, j):
        return pl.ds(pl.multiple_of((half * chunks + j) * HD, HD), HD)

    def history_span(source):
        return pl.ds(pl.multiple_of(source * history_rows, history_rows), history_rows)

    def fresh_span(base, source):
        return pl.ds(pl.multiple_of(base + source * local_rows, local_rows), local_rows)

    def query_span(source):
        return pl.ds(
            pl.multiple_of((camp * members + source) * local_rows, local_rows), local_rows
        )

    camp_span = pl.ds(pl.multiple_of(camp * camp_rows, camp_rows), camp_rows)
    far_span = pl.ds(pl.multiple_of((1 - camp) * camp_rows, camp_rows), camp_rows)

    def places(j, source):
        return (
            kv.at[j, core, history_span(source), :],
            kv.at[j, :, fresh_span(own_base, source), :],
            queries.at[j, query_span(source), :],
        )

    def wholes(j):
        return (
            kv.at[j, core, 0:camp_history, :],
            kv.at[j, :, own_base : own_base + camp_rows, :],
            queries.at[j, camp_span, :],
        )

    def origins(half, j):
        cols = columns(half, j)
        return (
            history_in.at[core, :, cols],
            fresh_in.at[:, 0, :, cols],
            query_in.at[0, :, cols],
        )

    def own_copies(half, j, device, slot, source, kinds):
        from_refs, to_refs = origins(half, j), places(j, source)
        return [
            remote(from_refs[k], to_refs[k], in_send.at[k, slot], in_recv.at[k, j], device)
            for k in kinds
        ]

    def forward(j, kinds):
        spots = places(j, side_seat)
        return [
            remote(spots[k], spots[k], forward_send.at[k, j], in_recv.at[k, j], mate_dev)
            for k in kinds
        ]

    def local_copies(j):
        from_refs, to_refs = origins(col, j), places(j, seat)
        return [
            pltpu.make_async_copy(from_refs[k], to_refs[k], in_recv.at[k, j]) for k in range(3)
        ]

    def await_bytes(ref, sem):
        pltpu.make_async_copy(ref, ref, sem).wait()

    def passed_history(j, which):
        place = kv.at[j, which, 0:camp_history, :]
        return remote(place, place, pass_send.at[0], pass_recv.at[0, j], twin)

    def passed_fresh(j):
        return remote(
            kv.at[j, :, own_base : own_base + camp_rows, :],
            kv.at[j, :, other_base : other_base + camp_rows, :],
            pass_send.at[1],
            pass_recv.at[1, j],
            twin,
        )

    def mirrored_query(j, span):
        place = queries.at[j, span, :]
        return remote(place, place, query_send, query_recv.at[j], mirror_dev)

    def swapped(j, piece):
        rows = pl.ds(piece * piece_rows, piece_rows)
        return (
            remote(
                part_send.at[j, rows, :],
                part_recv.at[j, rows, :],
                swap_send.at[0],
                swap_recv.at[0, j, piece],
                mirror_dev,
            ),
            remote(
                stat_send.at[j, :, rows],
                stat_recv.at[j, :, rows],
                swap_send.at[1],
                swap_recv.at[1, j, piece],
                mirror_dev,
            ),
        )

    def spread(half, j, piece):
        place = gathered.at[half * chunks + j, pl.ds(piece * piece_rows, piece_rows), :]
        return [
            remote(
                place,
                place,
                gather_send.at[way],
                gather_recv.at[half * chunks + j, piece],
                device,
            )
            for way, device in enumerate((side_dev, mate_dev))
        ]

    def block_rows(block):
        return pl.ds(pl.multiple_of(block * BLK, BLK), BLK)

    gate_copy = pltpu.make_async_copy(gate_in, gate, gate_sem)
    unit = math.log2(math.e) / math.sqrt(HD)

    def prepare_bias():
        live = blocks_ref[0] * BLK
        positions = camp * camp_history + lax.broadcasted_iota(
            jnp.int32, (1, camp_history), 1
        )
        history_bias = jnp.where(positions < live, 0.0, NEGATIVE)
        for block in range(block_count):
            bias[block : block + 1, 0:camp_history] = history_bias
            for part in range(2):
                for near in range(camp_blocks):
                    column = part * block_count + camp * camp_blocks + near
                    shown = jnp.full((1, BLK), mask_ref[0, block, column], jnp.int32)
                    begin = camp_history + part * camp_rows + near * BLK
                    bias[block : block + 1, begin : begin + BLK] = jnp.where(
                        shown > 0, 0.0, NEGATIVE
                    )

    def attend(j, piece):
        rows = pl.ds(piece * piece_rows, piece_rows)
        scores = lax.dot_general(
            queries[j, rows, :],
            kv[j, 0],
            (((1,), (1,)), ((), ())),
            preferred_element_type=jnp.float32,
        )
        peaks, sums, parts = [], [], []
        for place in range(piece_blocks):
            block = piece * piece_blocks + place
            part = scores[place * BLK : (place + 1) * BLK] * unit + bias[block : block + 1, :]
            peak = jnp.max(part, axis=1, keepdims=True)
            part = jnp.exp2(part - peak)
            peaks.append(peak)
            sums.append(jnp.sum(part, axis=1, keepdims=True))
            parts.append(part.astype(jnp.bfloat16))
        output = jnp.dot(
            jnp.concatenate(parts, axis=0), kv[j, 1], preferred_element_type=jnp.float32
        )
        output = output / jnp.concatenate(sums, axis=0)
        own_part[j, rows, :] = output
        part_send[j, rows, :] = output.astype(jnp.bfloat16)
        for place in range(piece_blocks):
            begin = piece * piece_rows + place * BLK
            level = jnp.broadcast_to(peaks[place] + jnp.log2(sums[place]), (BLK, BLK))
            own_lse[j, begin : begin + BLK, :] = level
            stat_send[j, :, begin : begin + BLK] = level.T[0:8, :]

    def combine(j, piece):
        for block in range(piece * piece_blocks, (piece + 1) * piece_blocks):
            rows = pl.ds(block * BLK, BLK)
            mine = own_lse[j, rows, :]
            theirs = jnp.broadcast_to(stat_recv[j, 0:1, rows], (BLK, BLK)).T
            top = jnp.maximum(mine, theirs)
            first = jnp.exp2(mine - top)
            second = jnp.exp2(theirs - top)
            mixed = own_part[j, rows, :] * first + part_recv[j, rows, :].astype(
                jnp.float32
            ) * second
            gathered[col * chunks + j, rows, :] = (mixed / (first + second)).astype(
                jnp.bfloat16
            )

    def project(j, halves, last):
        for piece in range(PIECES):
            for half in halves:
                spread(half, j, piece)[0].wait_recv()

            rows = pl.ds(piece * piece_rows, piece_rows)
            left = jnp.concatenate(
                [gathered[j, rows, :], gathered[chunks + j, rows, :]], axis=1
            )
            right = jnp.concatenate([weight[0, j], weight[1, j]], axis=0)
            part = jnp.dot(left, right, preferred_element_type=jnp.float32)
            part = part + total[rows, :]
            if last:
                factor = gate[pl.ds(level_ref[0], 1), :]
                out_ref[0, rows, :] = (part * factor).astype(out_ref.dtype)
            else:
                total[rows, :] = part

    def every(body, count=chunks, first=0):
        def step(j, carry):
            body(j)
            return carry

        lax.fori_loop(first, count, step, 0)

    def start(copies):
        for copy in copies:
            copy.start()

    weight_copy = pltpu.make_async_copy(weight_in, weight, weight_sem)
    scalar_copies = [
        pltpu.make_async_copy(source, target, scalar_sem.at[place])
        for place, (source, target) in enumerate(
            ((mask_in, mask_ref), (blocks_in, blocks_ref), (level_in, level_ref))
        )
    ]
    own_half = gathered.at[pl.ds(pl.multiple_of(col * chunks, chunks), chunks)]

    def await_own(slot):
        await_bytes(kv.at[:, 0, 0:history_rows, :], in_send.at[0, slot])
        await_bytes(kv.at[:, :, 0:local_rows, :], in_send.at[1, slot])
        await_bytes(queries.at[:, 0:local_rows, :], in_send.at[2, slot])

    @pl.when(inner)
    def _():
        def ask(j):
            start(own_copies(1 - col, j, side_dev, 0, seat, ASKED))

        def begin(j):
            start(own_copies(1 - col, j, side_dev, 0, seat, ROWS))
            pl.when(j + EARLY < chunks)(lambda: ask(j + EARLY))

        start(own_copies(1 - col, 0, side_dev, 0, seat, ROWS))
        every(ask, EARLY + 1)
        every(begin, SIDE_AHEAD, 1)
        start(scalar_copies)
        every(lambda j: start(local_copies(j)))
        weight_copy.start()
        gate_copy.start()
        total[...] = jnp.zeros_like(total)
        for copy in scalar_copies:
            copy.wait()
        prepare_bias()

        def answer(j):
            await_bytes(wholes(j)[2], in_recv.at[2, j])
            mirrored_query(j, camp_span).start()

        every(answer, EARLY)

        def take(j):
            await_bytes(wholes(j)[0], in_recv.at[0, j])
            passed_history(j, core).start()
            await_bytes(wholes(j)[1], in_recv.at[1, j])
            passed_fresh(j).start()
            pl.when(j + SIDE_AHEAD < chunks)(lambda: begin(j + SIDE_AHEAD))
            pl.when(j + EARLY < chunks)(lambda: answer(j + EARLY))

        def work(j):
            mirrored_query(j, far_span).wait_recv()
            passed_history(j, 1 - core).wait_recv()
            passed_fresh(j).wait_recv()
            for piece in range(PIECES):
                attend(j, piece)
                start(swapped(j, piece))

        def merge(j):
            for piece in range(PIECES):
                for copy in swapped(j, piece):
                    copy.wait_recv()
                combine(j, piece)
                start(spread(col, j, piece))

        def round_of(step):
            pl.when(step == INNER_LAG)(weight_copy.wait)
            pl.when(step < chunks)(lambda: take(step))
            pl.when((step >= COMBINE_LAG) & (step < chunks + COMBINE_LAG))(
                lambda: merge(step - COMBINE_LAG)
            )
            pl.when(step >= INNER_LAG)(
                lambda: project(step - INNER_LAG, (1 - col,), False)
            )
            pl.when(step < chunks)(lambda: work(step))

        every(round_of, chunks - 1 + INNER_LAG)
        gate_copy.wait()
        project(chunks - 1, (1 - col,), True)
        await_own(0)
        await_bytes(kv.at[:, 0, 0:camp_history, :], pass_send.at[0])
        await_bytes(kv.at[:, :, 0:camp_rows, :], pass_send.at[1])
        await_bytes(queries.at[:, 0:camp_rows, :], query_send)
        await_bytes(part_send, swap_send.at[0])
        await_bytes(stat_send, swap_send.at[1])
        await_bytes(own_half, gather_send.at[0])
        await_bytes(own_half, gather_send.at[1])

    @pl.when(jnp.logical_not(inner))
    def _():
        def ask(j):
            start(own_copies(1 - col, j, side_dev, 1, seat, ASKED))
            start(own_copies(col, j, mate_dev, 0, seat, ASKED))

        def begin(j):
            start(own_copies(col, j, mate_dev, 0, seat, ROWS))

        def begin_side(j):
            start(own_copies(1 - col, j, side_dev, 1, seat, ROWS))
            pl.when(j + EARLY < chunks)(lambda: ask(j + EARLY))

        start(own_copies(1 - col, 0, side_dev, 1, seat, ROWS))
        begin(0)
        every(ask, EARLY + 1)
        every(begin, AHEAD, 1)
        every(begin_side, SIDE_AHEAD, 1)
        scalar_copies[2].start()
        weight_copy.start()
        gate_copy.start()
        total[...] = jnp.zeros_like(total)

        def pass_on(j, kinds):
            arrivals = own_copies(col, j, side_dev, 1, side_seat, kinds)
            copies = forward(j, kinds)
            for arrival, copy in zip(arrivals, copies):
                arrival.wait_recv()
                copy.start()

        every(lambda j: pass_on(j, ASKED), EARLY)

        def hand_on(j):
            pass_on(j, ROWS)
            pl.when(j + AHEAD < chunks)(lambda: begin(j + AHEAD))
            pl.when(j + SIDE_AHEAD < chunks)(lambda: begin_side(j + SIDE_AHEAD))
            pl.when(j + EARLY < chunks)(lambda: pass_on(j + EARLY, ASKED))

        def settle(j):
            for copy in forward(j, ROWS + ASKED):
                copy.wait_send()

        def relay(j):
            for piece in range(PIECES):
                copy = spread(col, j, piece)[0]
                copy.wait_recv()
                copy.start()

        def round_of(step):
            pl.when(step == OUTER_LAG)(weight_copy.wait)
            pl.when(step < chunks)(lambda: hand_on(step))
            pl.when((step >= THROTTLE) & (step < chunks + THROTTLE))(
                lambda: settle(step - THROTTLE)
            )
            pl.when((step >= RELAY_LAG) & (step < chunks + RELAY_LAG))(
                lambda: relay(step - RELAY_LAG)
            )
            pl.when(step >= OUTER_LAG)(
                lambda: project(step - OUTER_LAG, (1 - col,), False)
            )

        every(round_of, chunks - 1 + OUTER_LAG)
        gate_copy.wait()
        scalar_copies[2].wait()
        project(chunks - 1, (1 - col,), True)
        await_own(0)
        await_own(1)
        await_bytes(own_half, gather_send.at[0])


def on_device_fused(
    query, stretch_kv, history_kv, block_mask, noise_level, history_blocks, out_weight, gate_table
):
    n = lax.axis_size("tp")
    chunks = H // 2
    local_rows, history_rows = query.shape[1], history_kv.shape[1]
    row_count = n * local_rows
    key_count = (n * history_rows + 2 * row_count) // 2
    wide = out_weight.shape[1]
    block_count = block_mask.shape[1]
    vector = pl.BlockSpec(memory_space=pltpu.VMEM)
    dma = pltpu.SemaphoreType.DMA
    return pl.pallas_call(
        functools.partial(fused_kernel, n, chunks),
        out_shape=pltpu.VMEM((1, row_count, wide), jnp.bfloat16),
        in_specs=[pl.BlockSpec(memory_space=pltpu.HBM)] * 8,
        out_specs=vector,
        scratch_shapes=[
            pltpu.VMEM((chunks, 2, key_count, HD), jnp.bfloat16),
            pltpu.VMEM((chunks, row_count, HD), jnp.bfloat16),
            pltpu.VMEM((chunks, row_count, HD), jnp.float32),
            pltpu.VMEM((chunks, row_count, HD), jnp.float32),
            pltpu.VMEM((chunks, row_count, HD), jnp.bfloat16),
            pltpu.VMEM((chunks, row_count, HD), jnp.bfloat16),
            pltpu.VMEM((chunks, 8, row_count), jnp.float32),
            pltpu.VMEM((chunks, 8, row_count), jnp.float32),
            pltpu.VMEM((2 * chunks, row_count, HD), jnp.bfloat16),
            pltpu.VMEM((2, chunks, HD, wide), jnp.bfloat16),
            pltpu.VMEM(gate_table.shape, jnp.float32),
            pltpu.VMEM((block_count, key_count), jnp.float32),
            pltpu.VMEM((row_count, wide), jnp.float32),
            pltpu.SMEM(block_mask.shape, jnp.int32),
            pltpu.SMEM(history_blocks.shape, jnp.int32),
            pltpu.SMEM(noise_level.shape, jnp.int32),
            dma((3, 2)),
            dma((3, chunks)),
            dma((3, chunks)),
            dma((2,)),
            dma((2, chunks)),
            dma,
            dma((chunks,)),
            dma((2,)),
            dma((2, chunks, PIECES)),
            dma((2,)),
            dma((2 * chunks, PIECES)),
            dma,
            dma,
            dma((3,)),
        ],
        compiler_params=pltpu.CompilerParams(
            collective_id=0, has_side_effects=True, vmem_limit_bytes=63 * 1024 * 1024
        ),
    )(
        block_mask,
        history_blocks,
        noise_level,
        query,
        stretch_kv,
        history_kv,
        out_weight.reshape(2, chunks, HD, wide),
        gate_table,
    )


def solution(mesh):
    count = mesh.shape["tp"]
    fits = H % 2 == 0 and count // 2 == 4 and count % 2 == 0 and mesh.shape["stretch"] == 2
    return jax.shard_map(
        on_device_fused if fits else on_device,
        mesh=mesh,
        in_specs=(
            P(("rep", "stretch"), "tp", None),
            P(None, ("rep", "stretch"), "tp", None),
            P(None, ("rep", "tp"), None),
            P(("rep", "stretch"), None, None),
            P(("rep", "stretch")),
            P("rep"),
            P(None, "tp"),
            P(None, "tp"),
        ),
        out_specs=P(("rep", "stretch"), None, "tp"),
        check_vma=False,
    )
```

```python
import functools
import math

import jax
import jax.numpy as jnp
from jax import lax
from jax.experimental import pallas as pl
from jax.experimental.pallas import tpu as pltpu
from jax.sharding import PartitionSpec as P

H = 24
HD = 128
BLK = 128


NEGATIVE = -1e30


def shifted(value, axis, steps):
    count = lax.axis_size(axis)
    first, last = (max(0, -steps), min(count, count - steps))
    return lax.ppermute(value, axis, [(source, source + steps) for source in range(first, last)])


def head_block(queries, key_rows, value_rows, allowed):
    key_count = key_rows.shape[0]
    head_count = queries.shape[1]
    key_heads = key_rows.reshape(key_count, head_count, HD)
    scores = jnp.einsum("qhd,khd->qhk", queries, key_heads, preferred_element_type=jnp.float32) * (
        1.0 / math.sqrt(HD)
    )
    scores = jnp.where(allowed[:, None, :], scores, NEGATIVE)
    row_peak = jnp.max(scores, axis=2)
    weights = jnp.where(allowed[:, None, :], jnp.exp(scores - row_peak[:, :, None]), 0.0)
    weight_sum = jnp.sum(weights, axis=2)
    output = None
    value_heads = value_rows.reshape(key_count, head_count, HD).astype(jnp.float32)
    output = jnp.einsum("qhk,khd->qhd", weights, value_heads, precision=lax.Precision.HIGHEST)
    return (row_peak, weight_sum, output)


def combine(earlier, later):
    row_peak = jnp.maximum(earlier[0], later[0])
    scale_one = jnp.exp(earlier[0] - row_peak)
    scale_two = jnp.exp(later[0] - row_peak)
    weight_sum = earlier[1] * scale_one + later[1] * scale_two
    output = None
    output = earlier[2] * scale_one[:, :, None] + later[2] * scale_two[:, :, None]
    return (row_peak, weight_sum, output)


def column_table(columns, block_count):
    return (columns[:, None] == jnp.arange(2 * block_count, dtype=jnp.int32)[None, :]).astype(
        jnp.float32
    )


def attend_all(
    queries,
    query_positions,
    fresh_keys,
    fresh_values,
    fresh_hot,
    mask_table,
    history_pair,
    history_live,
    span,
):
    row_count = queries.shape[0]
    head_count = queries.shape[1]
    block_count = mask_table.shape[0]
    query_hot = (
        (query_positions // BLK)[:, None] == jnp.arange(block_count, dtype=jnp.int32)[None, :]
    ).astype(jnp.float32)
    fresh_allowed = jnp.dot(jnp.dot(query_hot, mask_table), fresh_hot.T) > 0.5
    base_peak = jnp.full((row_count, head_count), NEGATIVE, jnp.float32)
    skipped = (
        base_peak,
        jnp.zeros((row_count, head_count), jnp.float32),
        jnp.zeros((row_count, head_count, HD), jnp.float32),
    )
    result = head_block(queries, fresh_keys, fresh_values, fresh_allowed)
    for sub_block in range(history_pair.shape[1] // span):
        lower_row = sub_block * span
        key_rows = history_pair[0, lower_row : lower_row + span]
        value_rows = history_pair[1, lower_row : lower_row + span]
        live_rows = history_live[lower_row : lower_row + span]
        allowed = jnp.broadcast_to(live_rows[None, :], (row_count, span))
        block_part = lax.cond(
            jnp.any(live_rows),
            lambda: head_block(queries, key_rows, value_rows, allowed),
            lambda: skipped,
        )
        result = combine(result, block_part)
    return result


def on_device(
    query, stretch_kv, history_kv, block_mask, noise_level, history_blocks, out_weight, gate_table
):
    tp_count = lax.axis_size("tp")
    tp_index = lax.axis_index("tp")
    local_rows = query.shape[1]
    feature_width = query.shape[2]
    history_rows = history_kv.shape[1]
    block_count = block_mask.shape[1]
    own_pair = stretch_kv[:, 0]
    older_pair = shifted(own_pair, "stretch", 1)
    mask_table = block_mask[0].astype(jnp.float32)
    live_limit = history_blocks[0] * BLK
    fresh_keys = jnp.concatenate([older_pair[0], own_pair[0]], 0)
    fresh_values = jnp.concatenate([older_pair[1], own_pair[1]], 0)
    own_positions = tp_index * local_rows + jnp.arange(local_rows, dtype=jnp.int32)
    fresh_hot = column_table(
        jnp.concatenate([own_positions // BLK, block_count + own_positions // BLK], 0), block_count
    )
    history_positions = tp_index * history_rows + jnp.arange(history_rows, dtype=jnp.int32)
    history_live = history_positions < live_limit
    piece = lax.all_gather(query[0], "tp", axis=0, tiled=True)
    row_count = piece.shape[0]
    positions = jnp.arange(row_count, dtype=jnp.int32)
    row_peak, weight_sum, output = attend_all(
        piece.reshape(row_count, H, HD),
        positions,
        fresh_keys,
        fresh_values,
        fresh_hot,
        mask_table,
        history_kv,
        history_live,
        BLK,
    )
    got_outputs, got_peaks, got_sums = (
        lax.all_to_all(
            output.reshape(tp_count, local_rows, H, HD),
            "tp",
            split_axis=0,
            concat_axis=0,
            tiled=True,
        ),
        lax.all_to_all(
            row_peak.reshape(tp_count, local_rows, H), "tp", split_axis=0, concat_axis=0, tiled=True
        ),
        lax.all_to_all(
            weight_sum.reshape(tp_count, local_rows, H),
            "tp",
            split_axis=0,
            concat_axis=0,
            tiled=True,
        ),
    )
    overall = jnp.max(got_peaks, axis=0)
    factor = jnp.exp(got_peaks - overall[None])
    merged_sum = jnp.sum(got_sums * factor, axis=0)
    merged = jnp.sum(got_outputs * factor[:, :, :, None], axis=0) / merged_sum[:, :, None]
    attended = merged.reshape(local_rows, feature_width).astype(jnp.bfloat16)
    projected = jnp.dot(
        lax.all_gather(attended, "tp", axis=0, tiled=True),
        out_weight,
        preferred_element_type=jnp.float32,
    )
    level_hot = (jnp.arange(gate_table.shape[0], dtype=jnp.int32) == noise_level[0]).astype(
        jnp.float32
    )[None, :]
    gate_row = jnp.dot(level_hot, gate_table, precision=lax.Precision.HIGHEST)
    return (projected * gate_row).astype(jnp.bfloat16)[None]


MESH = pl.DeviceIdType.MESH
ROWS = (0, 1)
ASKED = (2,)
PIECES = 2
AHEAD = 1
SIDE_AHEAD = 6
THROTTLE = 2
EARLY = 5
COMBINE_LAG = 2
INNER_LAG = 4
RELAY_LAG = 5
OUTER_LAG = 7


def fused_kernel(
    n,
    chunks,
    mask_in,
    blocks_in,
    level_in,
    query_in,
    fresh_in,
    history_in,
    weight_in,
    gate_in,
    out_ref,
    kv,
    queries,
    own_part,
    own_lse,
    part_send,
    part_recv,
    stat_send,
    stat_recv,
    gathered,
    weight,
    gate,
    bias,
    total,
    mask_ref,
    blocks_ref,
    level_ref,
    in_send,
    in_recv,
    forward_send,
    pass_send,
    pass_recv,
    query_send,
    query_recv,
    swap_send,
    swap_recv,
    gather_send,
    gather_recv,
    weight_sem,
    gate_sem,
    scalar_sem,
):
    me = lax.axis_index("tp")
    core = lax.axis_index("stretch")
    twin = {"stretch": 1 - core}
    line = n // 2
    spot, col = me // 2, me % 2
    members = n // 2
    camp = me // members
    seat = me % members
    inner = (spot > 0) & (spot < line - 1)
    mate_spot = spot + 1 - 2 * (spot % 2)
    side_dev = {"tp": me + 1 - 2 * col}
    mate_dev = {"tp": 2 * mate_spot + col}
    mirror_dev = {"tp": 2 * (line - 1 - spot) + col}
    side_seat = seat + 1 - 2 * col

    local_rows = query_in.shape[1]
    history_rows = history_in.shape[1]
    row_count = n * local_rows
    camp_rows = members * local_rows
    camp_history = members * history_rows
    other_base = camp_history
    own_base = camp_history + camp_rows
    block_count = mask_in.shape[1]
    camp_blocks = block_count // 2
    piece_blocks = block_count // PIECES
    piece_rows = piece_blocks * BLK
    wide = out_ref.shape[2]
    swap_rows = piece_rows + 2 * 8 * piece_rows // HD

    barrier = pltpu.get_barrier_semaphore()

    def greet(devices):
        for device in devices:
            pl.semaphore_signal(barrier, inc=1, device_id=device, device_id_type=MESH)

    greet((side_dev, mate_dev))
    pl.when(inner)(lambda: greet((mirror_dev, twin)))
    pl.semaphore_wait(barrier, jnp.where(inner, 4, 2))

    def remote(source, target, send, recv, device):
        return pltpu.make_async_remote_copy(
            src_ref=source,
            dst_ref=target,
            send_sem=send,
            recv_sem=recv,
            device_id=device,
            device_id_type=MESH,
        )

    def columns(half, j):
        return pl.ds(pl.multiple_of((half * chunks + j) * HD, HD), HD)

    def history_span(source):
        return pl.ds(pl.multiple_of(source * history_rows, history_rows), history_rows)

    def fresh_span(base, source):
        return pl.ds(pl.multiple_of(base + source * local_rows, local_rows), local_rows)

    def query_span(source):
        return pl.ds(
            pl.multiple_of((camp * members + source) * local_rows, local_rows), local_rows
        )

    camp_span = pl.ds(pl.multiple_of(camp * camp_rows, camp_rows), camp_rows)
    far_span = pl.ds(pl.multiple_of((1 - camp) * camp_rows, camp_rows), camp_rows)

    def places(j, source):
        return (
            kv.at[j, core, history_span(source), :],
            kv.at[j, :, fresh_span(own_base, source), :],
            queries.at[j, query_span(source), :],
        )

    def wholes(j):
        return (
            kv.at[j, core, 0:camp_history, :],
            kv.at[j, :, own_base : own_base + camp_rows, :],
            queries.at[j, camp_span, :],
        )

    def origins(half, j):
        cols = columns(half, j)
        return (
            history_in.at[core, :, cols],
            fresh_in.at[:, 0, :, cols],
            query_in.at[0, :, cols],
        )

    def own_copies(half, j, device, slot, source, kinds):
        from_refs, to_refs = origins(half, j), places(j, source)
        return [
            remote(from_refs[k], to_refs[k], in_send.at[k, slot], in_recv.at[k, j], device)
            for k in kinds
        ]

    def forward(j, kinds):
        spots = places(j, side_seat)
        return [
            remote(spots[k], spots[k], forward_send.at[k, j], in_recv.at[k, j], mate_dev)
            for k in kinds
        ]

    def local_copies(j):
        from_refs, to_refs = origins(col, j), places(j, seat)
        return [
            pltpu.make_async_copy(from_refs[k], to_refs[k], in_recv.at[k, j]) for k in range(3)
        ]

    def await_bytes(ref, sem):
        pltpu.make_async_copy(ref, ref, sem).wait()

    def passed_history(j, which):
        place = kv.at[j, which, 0:camp_history, :]
        return remote(place, place, pass_send.at[0], pass_recv.at[0, j], twin)

    def passed_fresh(j):
        return remote(
            kv.at[j, :, own_base : own_base + camp_rows, :],
            kv.at[j, :, other_base : other_base + camp_rows, :],
            pass_send.at[1],
            pass_recv.at[1, j],
            twin,
        )

    def mirrored_query(j, span):
        place = queries.at[j, span, :]
        return remote(place, place, query_send, query_recv.at[j], mirror_dev)

    def swapped(j, piece):
        rows = pl.ds(piece * piece_rows, piece_rows)
        return (
            remote(
                part_send.at[j, rows, :],
                part_recv.at[j, rows, :],
                swap_send.at[0],
                swap_recv.at[j, piece],
                mirror_dev,
            ),
            remote(
                stat_send.at[j, :, rows],
                stat_recv.at[j, :, rows],
                swap_send.at[1],
                swap_recv.at[j, piece],
                mirror_dev,
            ),
        )

    def spread(half, j, piece):
        place = gathered.at[half * chunks + j, pl.ds(piece * piece_rows, piece_rows), :]
        return [
            remote(
                place,
                place,
                gather_send.at[way],
                gather_recv.at[half * chunks + j, piece],
                device,
            )
            for way, device in enumerate((side_dev, mate_dev))
        ]

    def block_rows(block):
        return pl.ds(pl.multiple_of(block * BLK, BLK), BLK)

    gate_copy = pltpu.make_async_copy(gate_in, gate, gate_sem)
    unit = math.log2(math.e) / math.sqrt(HD)

    def prepare_bias():
        live = blocks_ref[0] * BLK
        positions = camp * camp_history + lax.broadcasted_iota(
            jnp.int32, (1, camp_history), 1
        )
        history_bias = jnp.where(positions < live, 0.0, NEGATIVE)
        for block in range(block_count):
            bias[block : block + 1, 0:camp_history] = history_bias
            for part in range(2):
                for near in range(camp_blocks):
                    column = part * block_count + camp * camp_blocks + near
                    shown = jnp.full((1, BLK), mask_ref[0, block, column], jnp.int32)
                    begin = camp_history + part * camp_rows + near * BLK
                    bias[block : block + 1, begin : begin + BLK] = jnp.where(
                        shown > 0, 0.0, NEGATIVE
                    )

    def attend(j, piece):
        rows = pl.ds(piece * piece_rows, piece_rows)
        scores = lax.dot_general(
            queries[j, rows, :],
            kv[j, 0],
            (((1,), (1,)), ((), ())),
            preferred_element_type=jnp.float32,
        )
        peaks, sums, parts = [], [], []
        for place in range(piece_blocks):
            block = piece * piece_blocks + place
            part = scores[place * BLK : (place + 1) * BLK] * unit + bias[block : block + 1, :]
            peak = jnp.max(part, axis=1, keepdims=True)
            part = jnp.exp2(part - peak)
            peaks.append(peak)
            sums.append(jnp.sum(part, axis=1, keepdims=True))
            parts.append(part.astype(jnp.bfloat16))
        output = jnp.dot(
            jnp.concatenate(parts, axis=0), kv[j, 1], preferred_element_type=jnp.float32
        )
        output = output / jnp.concatenate(sums, axis=0)
        own_part[j, rows, :] = output
        part_send[j, rows, :] = output.astype(jnp.bfloat16)
        for place in range(piece_blocks):
            begin = piece * piece_rows + place * BLK
            level = jnp.broadcast_to(peaks[place] + jnp.log2(sums[place]), (BLK, BLK))
            own_lse[j, begin : begin + BLK, :] = level
            stat_send[j, :, begin : begin + BLK] = level.T[0:8, :]

    def combine(j, piece):
        for block in range(piece * piece_blocks, (piece + 1) * piece_blocks):
            rows = pl.ds(block * BLK, BLK)
            mine = own_lse[j, rows, :]
            theirs = jnp.broadcast_to(stat_recv[j, 0:1, rows], (BLK, BLK)).T
            top = jnp.maximum(mine, theirs)
            first = jnp.exp2(mine - top)
            second = jnp.exp2(theirs - top)
            mixed = own_part[j, rows, :] * first + part_recv[j, rows, :].astype(
                jnp.float32
            ) * second
            gathered[col * chunks + j, rows, :] = (mixed / (first + second)).astype(
                jnp.bfloat16
            )

    def project(j, halves, last):
        for piece in range(PIECES):
            for half in halves:
                spread(half, j, piece)[0].wait_recv()

            rows = pl.ds(piece * piece_rows, piece_rows)
            left = jnp.concatenate(
                [gathered[j, rows, :], gathered[chunks + j, rows, :]], axis=1
            )
            right = jnp.concatenate([weight[0, j], weight[1, j]], axis=0)
            part = jnp.dot(left, right, preferred_element_type=jnp.float32)
            part = part + total[rows, :]
            if last:
                factor = gate[pl.ds(level_ref[0], 1), :]
                out_ref[0, rows, :] = (part * factor).astype(out_ref.dtype)
            else:
                total[rows, :] = part

    def every(body, count=chunks, first=0):
        def step(j, carry):
            body(j)
            return carry

        lax.fori_loop(first, count, step, 0)

    def start(copies):
        for copy in copies:
            copy.start()

    weight_copy = pltpu.make_async_copy(weight_in, weight, weight_sem)
    scalar_copies = [
        pltpu.make_async_copy(source, target, scalar_sem.at[place])
        for place, (source, target) in enumerate(
            ((mask_in, mask_ref), (blocks_in, blocks_ref), (level_in, level_ref))
        )
    ]
    own_half = gathered.at[pl.ds(pl.multiple_of(col * chunks, chunks), chunks)]

    def await_own(slot):
        await_bytes(kv.at[:, 0, 0:history_rows, :], in_send.at[0, slot])
        await_bytes(kv.at[:, :, 0:local_rows, :], in_send.at[1, slot])
        await_bytes(queries.at[:, 0:local_rows, :], in_send.at[2, slot])

    @pl.when(inner)
    def _():
        def ask(j):
            start(own_copies(1 - col, j, side_dev, 0, seat, ASKED))

        def begin(j):
            start(own_copies(1 - col, j, side_dev, 0, seat, ROWS))
            pl.when(j + EARLY < chunks)(lambda: ask(j + EARLY))

        start(own_copies(1 - col, 0, side_dev, 0, seat, ROWS))
        every(ask, EARLY + 1)
        every(begin, SIDE_AHEAD, 1)
        start(scalar_copies)
        every(lambda j: start(local_copies(j)))
        weight_copy.start()
        gate_copy.start()
        total[...] = jnp.zeros_like(total)
        for copy in scalar_copies:
            copy.wait()
        prepare_bias()

        def answer(j):
            await_bytes(wholes(j)[2], in_recv.at[2, j])
            mirrored_query(j, camp_span).start()

        every(answer, EARLY)

        def take(j):
            await_bytes(wholes(j)[0], in_recv.at[0, j])
            passed_history(j, core).start()
            await_bytes(wholes(j)[1], in_recv.at[1, j])
            passed_fresh(j).start()
            pl.when(j + SIDE_AHEAD < chunks)(lambda: begin(j + SIDE_AHEAD))
            pl.when(j + EARLY < chunks)(lambda: answer(j + EARLY))

        def work(j):
            mirrored_query(j, far_span).wait_recv()
            passed_history(j, 1 - core).wait_recv()
            passed_fresh(j).wait_recv()
            for piece in range(PIECES):
                attend(j, piece)
                start(swapped(j, piece))

        def merge(j):
            for piece in range(PIECES):
                await_bytes(kv.at[0, 0, 0:swap_rows, :], swap_recv.at[j, piece])
                combine(j, piece)
                start(spread(col, j, piece)[::-1])

        def round_of(step):
            pl.when(step == INNER_LAG)(weight_copy.wait)
            pl.when(step < chunks)(lambda: take(step))
            pl.when((step >= COMBINE_LAG) & (step < chunks + COMBINE_LAG))(
                lambda: merge(step - COMBINE_LAG)
            )
            pl.when(step >= INNER_LAG)(
                lambda: project(step - INNER_LAG, (1 - col,), False)
            )
            pl.when(step < chunks)(lambda: work(step))

        every(round_of, chunks - 1 + INNER_LAG)
        gate_copy.wait()
        project(chunks - 1, (1 - col,), True)
        await_own(0)
        await_bytes(kv.at[:, 0, 0:camp_history, :], pass_send.at[0])
        await_bytes(kv.at[:, :, 0:camp_rows, :], pass_send.at[1])
        await_bytes(queries.at[:, 0:camp_rows, :], query_send)
        await_bytes(part_send, swap_send.at[0])
        await_bytes(stat_send, swap_send.at[1])
        await_bytes(own_half, gather_send.at[0])
        await_bytes(own_half, gather_send.at[1])

    @pl.when(jnp.logical_not(inner))
    def _():
        def ask(j):
            start(own_copies(1 - col, j, side_dev, 1, seat, ASKED))
            start(own_copies(col, j, mate_dev, 0, seat, ASKED))

        def begin(j):
            start(own_copies(col, j, mate_dev, 0, seat, ROWS))

        def begin_side(j):
            start(own_copies(1 - col, j, side_dev, 1, seat, ROWS))
            pl.when(j + EARLY < chunks)(lambda: ask(j + EARLY))

        start(own_copies(1 - col, 0, side_dev, 1, seat, ROWS))
        begin(0)
        every(ask, EARLY + 1)
        every(begin, AHEAD, 1)
        every(begin_side, SIDE_AHEAD, 1)
        scalar_copies[2].start()
        weight_copy.start()
        gate_copy.start()
        total[...] = jnp.zeros_like(total)

        def pass_on(j, kinds):
            arrivals = own_copies(col, j, side_dev, 1, side_seat, kinds)
            copies = forward(j, kinds)
            for arrival, copy in zip(arrivals, copies):
                arrival.wait_recv()
                copy.start()

        every(lambda j: pass_on(j, ASKED), EARLY)

        def hand_on(j):
            pass_on(j, ROWS)
            pl.when(j + AHEAD < chunks)(lambda: begin(j + AHEAD))
            pl.when(j + SIDE_AHEAD < chunks)(lambda: begin_side(j + SIDE_AHEAD))
            pl.when(j + EARLY < chunks)(lambda: pass_on(j + EARLY, ASKED))

        def settle(j):
            for copy in forward(j, ROWS + ASKED):
                copy.wait_send()

        def relay(j):
            for piece in range(PIECES):
                copy = spread(col, j, piece)[0]
                copy.wait_recv()
                copy.start()

        def round_of(step):
            pl.when(step == OUTER_LAG)(weight_copy.wait)
            pl.when(step < chunks)(lambda: hand_on(step))
            pl.when((step >= THROTTLE) & (step < chunks + THROTTLE))(
                lambda: settle(step - THROTTLE)
            )
            pl.when((step >= RELAY_LAG) & (step < chunks + RELAY_LAG))(
                lambda: relay(step - RELAY_LAG)
            )
            pl.when(step >= OUTER_LAG)(
                lambda: project(step - OUTER_LAG, (1 - col,), False)
            )

        every(round_of, chunks - 1 + OUTER_LAG)
        gate_copy.wait()
        scalar_copies[2].wait()
        project(chunks - 1, (1 - col,), True)
        await_own(0)
        await_own(1)
        await_bytes(own_half, gather_send.at[0])


def on_device_fused(
    query, stretch_kv, history_kv, block_mask, noise_level, history_blocks, out_weight, gate_table
):
    n = lax.axis_size("tp")
    chunks = H // 2
    local_rows, history_rows = query.shape[1], history_kv.shape[1]
    row_count = n * local_rows
    key_count = (n * history_rows + 2 * row_count) // 2
    wide = out_weight.shape[1]
    block_count = block_mask.shape[1]
    vector = pl.BlockSpec(memory_space=pltpu.VMEM)
    dma = pltpu.SemaphoreType.DMA
    return pl.pallas_call(
        functools.partial(fused_kernel, n, chunks),
        out_shape=pltpu.VMEM((1, row_count, wide), jnp.bfloat16),
        in_specs=[pl.BlockSpec(memory_space=pltpu.HBM)] * 8,
        out_specs=vector,
        scratch_shapes=[
            pltpu.VMEM((chunks, 2, key_count, HD), jnp.bfloat16),
            pltpu.VMEM((chunks, row_count, HD), jnp.bfloat16),
            pltpu.VMEM((chunks, row_count, HD), jnp.float32),
            pltpu.VMEM((chunks, row_count, HD), jnp.float32),
            pltpu.VMEM((chunks, row_count, HD), jnp.bfloat16),
            pltpu.VMEM((chunks, row_count, HD), jnp.bfloat16),
            pltpu.VMEM((chunks, 8, row_count), jnp.float32),
            pltpu.VMEM((chunks, 8, row_count), jnp.float32),
            pltpu.VMEM((2 * chunks, row_count, HD), jnp.bfloat16),
            pltpu.VMEM((2, chunks, HD, wide), jnp.bfloat16),
            pltpu.VMEM(gate_table.shape, jnp.float32),
            pltpu.VMEM((block_count, key_count), jnp.float32),
            pltpu.VMEM((row_count, wide), jnp.float32),
            pltpu.SMEM(block_mask.shape, jnp.int32),
            pltpu.SMEM(history_blocks.shape, jnp.int32),
            pltpu.SMEM(noise_level.shape, jnp.int32),
            dma((3, 2)),
            dma((3, chunks)),
            dma((3, chunks)),
            dma((2,)),
            dma((2, chunks)),
            dma,
            dma((chunks,)),
            dma((2,)),
            dma((chunks, PIECES)),
            dma((2,)),
            dma((2 * chunks, PIECES)),
            dma,
            dma,
            dma((3,)),
        ],
        compiler_params=pltpu.CompilerParams(
            collective_id=0, has_side_effects=True, vmem_limit_bytes=63 * 1024 * 1024
        ),
    )(
        block_mask,
        history_blocks,
        noise_level,
        query,
        stretch_kv,
        history_kv,
        out_weight.reshape(2, chunks, HD, wide),
        gate_table,
    )


def solution(mesh):
    count = mesh.shape["tp"]
    fits = H % 2 == 0 and count // 2 == 4 and count % 2 == 0 and mesh.shape["stretch"] == 2
    return jax.shard_map(
        on_device_fused if fits else on_device,
        mesh=mesh,
        in_specs=(
            P(("rep", "stretch"), "tp", None),
            P(None, ("rep", "stretch"), "tp", None),
            P(None, ("rep", "tp"), None),
            P(("rep", "stretch"), None, None),
            P(("rep", "stretch")),
            P("rep"),
            P(None, "tp"),
            P(None, "tp"),
        ),
        out_specs=P(("rep", "stretch"), None, "tp"),
        check_vma=False,
    )
```
